8 devices in a mesh: model: 1 (over z), replica: 2 (over y), fsdp: 4 (over x, core).
Axes of the slice: x: 2, y: 2, z: 1, core: 2. Of those that a mesh axis runs over, the one named last changes fastest.
Arguments:
- x_in: bfloat16 [3, 8192, 2048], P(None, ('model', 'replica', 'fsdp'))
- dy_out: bfloat16 [3, 8192, 2048], P(None, ('model', 'replica', 'fsdp'))
- lengths: int32 [3, 8], P(None, ('model', 'replica', 'fsdp'))
- w_up: bfloat16 [1, 2048, 8192], P(None, ('model', 'fsdp'))
- w_down: bfloat16 [1, 8192, 2048], P(None, ('model', 'fsdp'))
Outputs:
- output 1: float32 [1, 2048, 8192], P(None, ('model', 'fsdp'))
- output 2: float32 [1, 8192, 2048], P(None, ('model', 'fsdp'))
All inputs are finite; a program needn't handle non-finite values.
Results may differ from the reference program's by a relative error of at most 0.001.
Values are sent between devices in bfloat16 or wider.
A program may use at most 1 GiB of HBM per device.

```python
import jax
import jax.numpy as jnp
from jax import lax

D_MODEL = 2048
D_FF = 8192
N_LAYERS = 1
N_MICRO = 3
TOK_DEV = 1024
N_REPLICA = 2
N_FSDP = 4

GROUP_DEV = N_REPLICA * N_FSDP
TOKENS = GROUP_DEV * TOK_DEV


def setup_inputs(seed: int = 0, part: int = 0) -> dict:
    base_key = jax.random.fold_in(jax.random.key(seed), part)
    key_list = jax.random.split(base_key, 5)
    grad_scale = (N_MICRO * TOKENS) ** -0.5
    x_in = jax.random.normal(key_list[0], (N_MICRO, TOKENS, D_MODEL), jnp.float32).astype(jnp.bfloat16)
    dy_out = (jax.random.normal(key_list[1], (N_MICRO, TOKENS, D_MODEL), jnp.float32) * grad_scale).astype(jnp.bfloat16)
    lengths = jax.random.randint(key_list[2], (N_MICRO, GROUP_DEV), TOK_DEV // 4, TOK_DEV + 1, dtype=jnp.int32)
    lengths = lengths.at[0, 0].set(TOK_DEV).at[N_MICRO - 1, GROUP_DEV - 1].set(TOK_DEV // 4)
    w_up = (jax.random.normal(key_list[3], (N_LAYERS, D_MODEL, D_FF), jnp.float32) * D_MODEL ** -0.5).astype(jnp.bfloat16)
    w_down = (jax.random.normal(key_list[4], (N_LAYERS, D_FF, D_MODEL), jnp.float32) * D_FF ** -0.5).astype(jnp.bfloat16)
    return {"x_in": x_in, "dy_out": dy_out, "lengths": lengths, "w_up": w_up, "w_down": w_down}


def layer_forward(x_cur, weights):
    w_up_l, w_down_l = weights
    hidden = jnp.dot(x_cur, w_up_l, preferred_element_type=jnp.float32).astype(jnp.bfloat16)
    act_bf = jax.nn.gelu(hidden.astype(jnp.float32)).astype(jnp.bfloat16)
    x_next = (x_cur.astype(jnp.float32) + jnp.dot(act_bf, w_down_l, preferred_element_type=jnp.float32)).astype(jnp.bfloat16)
    return x_next, (x_cur, hidden)


def layer_backward(grad_x, item):
    w_up_l, w_down_l, x_cur, hidden = item
    act_f32, gelu_vjp = jax.vjp(jax.nn.gelu, hidden.astype(jnp.float32))
    act_bf = act_f32.astype(jnp.bfloat16)
    grad_act = jnp.dot(grad_x, w_down_l.T, preferred_element_type=jnp.float32)
    grad_hid = gelu_vjp(grad_act)[0].astype(jnp.bfloat16)
    gw_down = jnp.dot(act_bf.T, grad_x, preferred_element_type=jnp.float32)
    gw_up = jnp.dot(x_cur.T, grad_hid, preferred_element_type=jnp.float32)
    grad_prev = (grad_x.astype(jnp.float32) + jnp.dot(grad_hid, w_up_l.T, preferred_element_type=jnp.float32)).astype(jnp.bfloat16)
    return grad_prev, (gw_up, gw_down)


def reference(x_in, dy_out, lengths, w_up, w_down):
    n_blocks = N_MICRO * GROUP_DEV
    x_blocks = x_in.reshape(n_blocks, TOK_DEV, D_MODEL)
    dy_blocks = dy_out.reshape(n_blocks, TOK_DEV, D_MODEL)
    len_blocks = lengths.reshape(n_blocks)

    def block_grads(acc_pair, block_in):
        x_blk, dy_blk, len_blk = block_in
        _, saved_acts = lax.scan(layer_forward, x_blk, (w_up, w_down))
        token_mask = jnp.arange(TOK_DEV) < len_blk
        grad_top = jnp.where(token_mask[:, None], dy_blk, jnp.zeros_like(dy_blk))
        _, grads = lax.scan(layer_backward, grad_top, (w_up, w_down, saved_acts[0], saved_acts[1]), reverse=True)
        return (acc_pair[0] + grads[0], acc_pair[1] + grads[1]), None

    init_pair = (jnp.zeros((N_LAYERS, D_MODEL, D_FF), jnp.float32), jnp.zeros((N_LAYERS, D_FF, D_MODEL), jnp.float32))
    (grad_up, grad_down), _ = lax.scan(block_grads, init_pair, (x_blocks, dy_blocks, len_blocks))
    return grad_up, grad_down
```

```python
import jax
import jax.numpy as jnp
from jax import lax
from jax.experimental import pallas as pl
from jax.experimental.pallas import tpu as pltpu
from jax.sharding import PartitionSpec as P


D = 2048
TOK = 1024
MICRO = 3
BASE = 256
REST = TOK - BASE
TM = 128
NT = MICRO * REST // TM
RROWS = MICRO * REST + TM
CAP = 6
G = 4
M = G * TM
FB = 256
HB = FB // 2
NCH = D // FB
HALF = 1024
NSRC = 12
C1 = 0.7978845608028654
C3 = 0.044715
BF = jnp.bfloat16
F32 = jnp.float32


ANY = pl.BlockSpec(memory_space=pl.ANY)
SM = pl.BlockSpec(memory_space=pltpu.SMEM)
VM = pl.BlockSpec(memory_space=pltpu.VMEM)
MIB = 1024 * 1024

CORE = [(0, 1), (1, 0), (2, 3), (3, 2)]
XSWAP = [(0, 2), (2, 0), (1, 3), (3, 1)]
XDIAG = [(0, 3), (3, 0), (1, 2), (2, 1)]
YSWAP = [(0, 1), (1, 0)]
YDIAG = [(r * 4 + f, (1 - r) * 4 + (f ^ 1)) for r in range(2) for f in range(4)]


def core_swap(v):
    return lax.ppermute(v, "fsdp", CORE)


def x_swap(v):
    return lax.ppermute(v, "fsdp", XSWAP)


def x_diag(v):
    return lax.ppermute(v, "fsdp", XDIAG)


def y_swap(v):
    return lax.ppermute(v, "replica", YSWAP)


def y_diag(v):
    return lax.ppermute(v, ("replica", "fsdp"), YDIAG)


def cost(flops, nbytes):
    return pl.CostEstimate(flops=flops, bytes_accessed=nbytes, transcendentals=0)


def pack_rest(x_in, dy, rest, offs):
    def kern(rest_ref, offs_ref, x_ref, d_ref, out_ref, buf, zero, isem, osem, zsem):
        loads = []
        for k in range(MICRO):
            for a, ref in enumerate((x_ref, d_ref)):
                cp = pltpu.make_async_copy(ref.at[k, pl.ds(BASE, REST), :], buf.at[k, a], isem.at[k, a])
                cp.start()
                loads.append(cp)
        zero[...] = jnp.zeros_like(zero)
        for k in range(MICRO):
            n = rest_ref[k]
            for a in range(2):
                loads[2 * k + a].wait()
                for r in range(0, REST, TM):
                    row = lax.broadcasted_iota(jnp.int32, (TM, D), 0) + r
                    blk = buf[k, a, r : r + TM, :]
                    buf[k, a, r : r + TM, :] = jnp.where(row < n, blk, jnp.zeros_like(blk))
            o = pl.multiple_of(offs_ref[k], 16)
            cps = [
                pltpu.make_async_copy(buf.at[k, a], out_ref.at[a, pl.ds(o, REST), :], osem.at[a]) for a in range(2)
            ]
            for cp in cps:
                cp.start()
            for cp in cps:
                cp.wait()
        for o in (pl.multiple_of(offs_ref[MICRO], 16), MICRO * REST):
            cps = [pltpu.make_async_copy(zero, out_ref.at[a, pl.ds(o, TM), :], zsem.at[a]) for a in range(2)]
            for cp in cps:
                cp.start()
            for cp in cps:
                cp.wait()

    return pl.pallas_call(
        kern,
        in_specs=[SM, SM, ANY, ANY],
        out_specs=ANY,
        out_shape=jax.ShapeDtypeStruct((2, RROWS, D), BF),
        scratch_shapes=[
            pltpu.VMEM((MICRO, 2, REST, D), BF),
            pltpu.VMEM((TM, D), BF),
            pltpu.SemaphoreType.DMA((MICRO, 2)),
            pltpu.SemaphoreType.DMA((2,)),
            pltpu.SemaphoreType.DMA((2,)),
        ],
        compiler_params=pltpu.CompilerParams(vmem_limit_bytes=40 * MIB),
        cost_estimate=cost(15_000_000_000, 50_000_000),
        name="pack_rest",
    )(rest, offs, x_in, dy)


def build_send(own, sib, info):
    def kern(info_ref, own_ref, sib_ref, out_ref, buf, isem, osem):
        n, mine, shift = info_ref[0], info_ref[1], info_ref[2]

        def load(i, slot):
            @pl.when(i < mine)
            def _():
                r = pl.multiple_of(i * TM, TM)
                pltpu.make_async_copy(own_ref.at[:, pl.ds(r, TM), :], buf.at[slot], isem.at[slot]).start()

            @pl.when(i >= mine)
            def _():
                r = pl.multiple_of((i + shift) * TM, TM)
                pltpu.make_async_copy(sib_ref.at[:, pl.ds(r, TM), :], buf.at[slot], isem.at[slot]).start()

        def store(i, slot):
            r = pl.multiple_of(i * TM, TM)
            return pltpu.make_async_copy(buf.at[slot], out_ref.at[:, pl.ds(r, TM), :], osem.at[slot])

        for s in range(3):

            @pl.when(s < n)
            def _():
                load(s, s)

        def body(i, _):
            slot = lax.rem(i, 4)
            pltpu.make_async_copy(own_ref.at[:, pl.ds(0, TM), :], buf.at[slot], isem.at[slot]).wait()
            store(i, slot).start()

            @pl.when(i >= 1)
            def _():
                store(i - 1, lax.rem(i + 3, 4)).wait()

            @pl.when(i + 3 < n)
            def _():
                load(i + 3, lax.rem(i + 3, 4))

            return 0

        lax.fori_loop(0, n, body, 0)

        @pl.when(n > 0)
        def _():
            store(n - 1, lax.rem(n + 3, 4)).wait()

    return pl.pallas_call(
        kern,
        in_specs=[SM, ANY, ANY],
        out_specs=ANY,
        out_shape=jax.ShapeDtypeStruct((2, NT * TM, D), BF),
        scratch_shapes=[pltpu.VMEM((4, 2, TM, D), BF), pltpu.SemaphoreType.DMA((4,)), pltpu.SemaphoreType.DMA((4,))],
        cost_estimate=cost(10_000_000_000, 36_000_000),
        name="build_send",
    )(info, own, sib)


def gelu_and_slope(u):
    u2 = u * u
    t = jnp.tanh(u * (C1 + (C1 * C3) * u2))
    half = 0.5 + 0.5 * t
    act = u * half
    slope = half + (0.5 * u) * (1.0 - t * t) * (C1 + (3 * C1 * C3) * u2)
    return act, slope


def chunk_grads(j, tab, info, srcs, wus, wds, deps):
    def kern(tab_ref, info_ref, *refs):
        src = refs[:NSRC]
        wu_refs, wd_refs = refs[NSRC : NSRC + 4], refs[NSRC + 4 : NSRC + 6]
        refs = refs[NSRC + 6 + len(deps) :]
        keep_d, keep_u, send, xb, db, wub, wdb, gd, gu, sem, wsem, osem = refs
        groups, xi, f = info_ref[0], info_ref[1], info_ref[2]
        c0 = j * HB
        wcp = []
        for a in range(2):
            for k in range(4):
                rows = pl.ds(pl.multiple_of((f ^ k) * 512, 512), 512)
                wcp.append(
                    pltpu.make_async_copy(
                        wu_refs[k].at[a, :, pl.ds(c0, HB)], wub.at[rows, pl.ds(a * HB, HB)], wsem.at[k, a]
                    )
                )
            wcp.append(
                pltpu.make_async_copy(wd_refs[a].at[pl.ds(c0, HB), :], wdb.at[pl.ds(a * HB, HB), :], wsem.at[4, a])
            )
        for cp in wcp:
            cp.start()

        def pick(e, lo, hi, fn):
            if hi - lo == 1:
                fn(lo)
                return
            mid = (lo + hi) // 2

            @pl.when(e < mid * 32)
            def _():
                pick(e, lo, mid, fn)

            @pl.when(e >= mid * 32)
            def _():
                pick(e, mid, hi, fn)

        def issue(g, slot):
            for s in range(G):
                e = tab_ref[g * G + s]
                r = pl.multiple_of(lax.rem(e, 32) * TM, TM)

                def fetch(k):
                    rows = pl.ds(s * TM, TM)
                    pltpu.make_async_copy(src[k].at[0, pl.ds(r, TM), :], xb.at[slot, rows, :], sem.at[slot, 0]).start()
                    pltpu.make_async_copy(src[k].at[1, pl.ds(r, TM), :], db.at[slot, rows, :], sem.at[slot, 1]).start()

                pick(e, 0, NSRC, fetch)

        issue(0, 0)
        gd[...] = jnp.zeros_like(gd)
        gu[...] = jnp.zeros_like(gu)
        for cp in wcp:
            cp.wait()

        def body(g, _):
            slot = lax.rem(g, 2)

            @pl.when(g + 1 < groups)
            def _():
                issue(g + 1, 1 - slot)

            pltpu.make_async_copy(xb.at[slot], xb.at[slot], sem.at[slot, 0]).wait()
            pltpu.make_async_copy(db.at[slot], db.at[slot], sem.at[slot, 1]).wait()
            x, dy = xb[slot], db[slot]
            u = jnp.dot(x, wub[...], preferred_element_type=F32).astype(BF).astype(F32)
            da = lax.dot_general(dy, wdb[...], (((1,), (1,)), ((), ())), preferred_element_type=F32)
            act, slope = gelu_and_slope(u)
            dh = (da * slope).astype(BF)
            gd[...] += lax.dot_general(act.astype(BF), dy, (((0,), (0,)), ((), ())), preferred_element_type=F32)
            gu[...] += lax.dot_general(dh, x, (((0,), (0,)), ((), ())), preferred_element_type=F32)
            return 0

        lax.fori_loop(0, groups, body, 0)
        kc = pl.multiple_of(xi * HALF, HALF)
        sc = pl.multiple_of((1 - xi) * HALF, HALF)
        ocp = [
            (gd.at[pl.ds(HB, HB), :], send.at[pl.ds(0, HB), :]),
            (gu.at[pl.ds(0, HB), pl.ds(sc, HALF)], send.at[pl.ds(HB, HB), pl.ds(0, HALF)]),
            (gu.at[pl.ds(HB, HB), pl.ds(sc, HALF)], send.at[pl.ds(HB, HB), pl.ds(HALF, HALF)]),
            (gd.at[pl.ds(0, HB), :], keep_d),
            (gu.at[:, pl.ds(kc, HALF)], keep_u),
        ]
        ocp = [pltpu.make_async_copy(a, b, osem.at[i]) for i, (a, b) in enumerate(ocp)]
        for cp in ocp:
            cp.start()
        for cp in ocp:
            cp.wait()

    n_in = NSRC + 6 + len(deps)
    return pl.pallas_call(
        kern,
        in_specs=[SM, SM] + [ANY] * n_in,
        out_specs=[ANY] * 3,
        out_shape=[
            jax.ShapeDtypeStruct((HB, D), F32),
            jax.ShapeDtypeStruct((FB, HALF), F32),
            jax.ShapeDtypeStruct((FB, D), F32),
        ],
        scratch_shapes=[
            pltpu.VMEM((2, M, D), BF),
            pltpu.VMEM((2, M, D), BF),
            pltpu.VMEM((D, FB), BF),
            pltpu.VMEM((FB, D), BF),
            pltpu.VMEM((FB, D), F32),
            pltpu.VMEM((FB, D), F32),
            pltpu.SemaphoreType.DMA((2, 2)),
            pltpu.SemaphoreType.DMA((5, 2)),
            pltpu.SemaphoreType.DMA((5,)),
        ],
        compiler_params=pltpu.CompilerParams(vmem_limit_bytes=40 * MIB),
        cost_estimate=cost(8 * 8192 * D * FB, 70_000_000),
    )(tab, info, *srcs, *wus, *wds, *deps)


def finish(j, pos, keep_d, keep_u, recv, outs):
    first = outs is None

    def kern(pos_ref, kd, ku, rc, *refs):
        refs = refs if first else refs[2:]
        out_d, out_u, fd, fuc, fus, vd, vu, sem = refs
        y, xi, c = pos_ref[0], pos_ref[1], pos_ref[2]
        vd[...] = kd[...] + rc[0:HB, :]
        row = pl.multiple_of(y * HALF + j * HB, HB)
        cps = [
            pltpu.make_async_copy(vd, fd, sem.at[0]),
            pltpu.make_async_copy(vd, out_d.at[pl.ds(row, HB), :], sem.at[1]),
        ]
        for cp in cps:
            cp.start()
        vu[0] = (ku[0:HB, :] + rc[HB:FB, HALF:D]).T
        vu[1] = (ku[HB:FB, :] + rc[HB:FB, 0:HALF]).T
        mine = pl.ds(pl.multiple_of(c * 512, 512), 512)
        other = pl.ds(pl.multiple_of((1 - c) * 512, 512), 512)
        more = [
            pltpu.make_async_copy(vu.at[:, other, :], fus, sem.at[2]),
            pltpu.make_async_copy(vu.at[:, mine, :], fuc, sem.at[3]),
        ]
        for a in range(2):
            xa = xi if a == 0 else 1 - xi
            col = pl.multiple_of(((2 * xa + c) * 2 + y) * HALF + j * HB, HB)
            more.append(pltpu.make_async_copy(vu.at[a, mine, :], out_u.at[:, pl.ds(col, HB)], sem.at[4 + a]))
        for cp in more:
            cp.start()
        for cp in cps + more:
            cp.wait()

    shapes = [
        jax.ShapeDtypeStruct((D, D), F32),
        jax.ShapeDtypeStruct((512, 4 * D), F32),
        jax.ShapeDtypeStruct((HB, D), F32),
        jax.ShapeDtypeStruct((2, 512, HB), F32),
        jax.ShapeDtypeStruct((2, 512, HB), F32),
    ]
    extra = [] if first else list(outs)
    return pl.pallas_call(
        kern,
        in_specs=[SM, VM, VM, VM] + [ANY] * len(extra),
        out_specs=[ANY] * 5,
        out_shape=shapes,
        scratch_shapes=[pltpu.VMEM((HB, D), F32), pltpu.VMEM((2, HALF, HB), F32), pltpu.SemaphoreType.DMA((6,))],
        input_output_aliases={} if first else {4: 0, 5: 1},
        compiler_params=pltpu.CompilerParams(vmem_limit_bytes=24 * MIB),
        cost_estimate=cost(4_000_000_000, 9_000_000),
    )(pos, keep_d, keep_u, recv, *extra)


def store(j, pos, rd, ruc, ruy, rus, outs):
    def kern(pos_ref, d_ref, uc_ref, uy_ref, us_ref, _d, _u, out_d, out_u, vd, vu, isem, osem):
        y, xi, c = pos_ref[0], pos_ref[1], pos_ref[2]
        loads = [pltpu.make_async_copy(d_ref, vd, isem.at[0])]
        for k, r in enumerate((uc_ref, uy_ref, us_ref)):
            loads.append(pltpu.make_async_copy(r, vu.at[k], isem.at[1 + k]))
        for cp in loads:
            cp.start()
        row = pl.multiple_of((1 - y) * HALF + j * HB, HB)
        loads[0].wait()
        outc = [pltpu.make_async_copy(vd, out_d.at[pl.ds(row, HB), :], osem.at[0])]
        outc[0].start()
        for k, (cc, yy) in enumerate(((c, 1 - y), (1 - c, 1 - y), (1 - c, y))):
            loads[1 + k].wait()
            for a in range(2):
                xa = xi if a == 0 else 1 - xi
                col = pl.multiple_of(((2 * xa + cc) * 2 + yy) * HALF + j * HB, HB)
                cp = pltpu.make_async_copy(vu.at[k, a], out_u.at[:, pl.ds(col, HB)], osem.at[1 + 2 * k + a])
                cp.start()
                outc.append(cp)
        for cp in outc:
            cp.wait()

    return pl.pallas_call(
        kern,
        in_specs=[SM] + [ANY] * 6,
        out_specs=[ANY] * 2,
        out_shape=[jax.ShapeDtypeStruct((D, D), F32), jax.ShapeDtypeStruct((512, 4 * D), F32)],
        scratch_shapes=[
            pltpu.VMEM((HB, D), F32),
            pltpu.VMEM((3, 2, 512, HB), F32),
            pltpu.SemaphoreType.DMA((4,)),
            pltpu.SemaphoreType.DMA((7,)),
        ],
        input_output_aliases={5: 0, 6: 1},
        compiler_params=pltpu.CompilerParams(vmem_limit_bytes=16 * MIB),
        cost_estimate=cost(3_000_000_000, 5_000_000),
    )(pos, rd, ruc, ruy, rus, *outs)


def exchange_branch(n):
    def run(send, s1_y):
        s1_ys = core_swap(s1_y)
        mine, sibs = [], []
        for p in range(NT // CAP):
            k = min(max(n - p * CAP, 0), CAP)
            if k == 0:
                got = jnp.zeros((2, CAP * TM, D), BF)
                mine.append(got)
                sibs.append(got)
                continue
            got = y_swap(send[:, p * CAP * TM : (p * CAP + k) * TM, :])
            sib = core_swap(got)
            if k < CAP:
                pad = ((0, 0, 0), (0, (CAP - k) * TM, 0), (0, 0, 0))
                got = lax.pad(got, jnp.zeros((), BF), pad)
                sib = lax.pad(sib, jnp.zeros((), BF), pad)
            mine.append(got)
            sibs.append(sib)
        return (s1_ys, *mine, *sibs)

    return run


def solution(mesh):
    tok_spec = P(None, ("model", "replica", "fsdp"), None)
    len_spec = P(None, ("model", "replica", "fsdp"))
    w_spec = P(None, ("model", "fsdp"), None)

    def group_grads(x_in, dy, lengths, w_up, w_down):
        y, f = lax.axis_index("replica"), lax.axis_index("fsdp")
        xi, c = f // 2, f % 2
        w_up, w_down = w_up[0], w_down[0]

        s1 = jnp.stack([x_in[:, :BASE], dy[:, :BASE]]).reshape(2, MICRO * BASE, D)
        s1_y = y_swap(s1)

        def cols(xd, cd):
            own = lax.dynamic_slice(w_up, (0, ((2 * xd + cd) * 2 + y) * HALF), (512, HALF))
            oth = lax.dynamic_slice(w_up, (0, ((2 * (1 - xd) + cd) * 2 + y) * HALF), (512, HALF))
            return jnp.stack([own, oth])

        wd_own = lax.dynamic_slice(w_down, (y * HALF, 0), (HALF, D))
        from_x = x_swap(cols(1 - xi, c))
        from_d = x_diag(cols(1 - xi, 1 - c))
        wd_oth = x_swap(wd_own)
        from_s = core_swap(cols(xi, 1 - c))
        wus = (cols(xi, c), from_s, from_x, from_d)
        wds = (wd_own, wd_oth)

        lens = lax.all_gather(lengths[:, 0], ("replica", "fsdp")).astype(jnp.int32)
        rest = lens - BASE
        r16 = (rest + 15) // 16 * 16
        tiles = (jnp.sum(r16, axis=1) + TM - 1) // TM
        me = y * 4 + f
        my_rest = lax.dynamic_index_in_dim(rest, me, keepdims=False)
        my16 = lax.dynamic_index_in_dim(r16, me, keepdims=False)
        offs = jnp.concatenate([jnp.zeros((1,), jnp.int32), jnp.cumsum(my16)])
        both = tiles[0::2] + tiles[1::2]
        share = jnp.stack([(both + 1) // 2, both // 2], axis=1).reshape(8)
        n2 = jnp.max(share)

        def at(v, i):
            return lax.dynamic_index_in_dim(v, i, keepdims=False)

        t_own, t_sib = at(tiles, me), at(tiles, me ^ 1)
        h_own = at(share, me)
        h_y, h_ys = at(share, me ^ 4), at(share, me ^ 5)

        packed = pack_rest(x_in, dy, my_rest, offs)
        packed_s = core_swap(packed)
        s1_s = core_swap(s1)
        send2 = build_send(packed, packed_s, jnp.stack([h_own, t_own, t_sib - h_own]))

        i = jnp.arange(128)
        b1 = 24
        b2 = b1 + t_own
        b3 = b2 + t_sib
        b4 = b3 + h_y
        b5 = b4 + h_ys
        k3, k4 = i - b3, i - b4
        tab = jnp.where(i < b5, (9 + k4 // CAP) * 32 + k4 % CAP, 4 * 32 + NT)
        tab = jnp.where(i < b4, (6 + k3 // CAP) * 32 + k3 % CAP, tab)
        tab = jnp.where(i < b3, 5 * 32 + (i - b2), tab)
        tab = jnp.where(i < b2, 4 * 32 + (i - b1), tab)
        tab = jnp.where(i < b1, (i // 6) * 32 + i % 6, tab).astype(jnp.int32)
        info = jnp.stack([(b5 + G - 1) // G, xi, f]).astype(jnp.int32)
        pos = jnp.stack([y, xi, c]).astype(jnp.int32)

        s1_ys, *s2 = lax.switch(n2, [exchange_branch(n) for n in range(NT + 1)], send2, s1_y)
        srcs = (s1, s1_s, s1_y, s1_ys, packed, packed_s, *s2)

        outs = None
        fin = []
        for j in range(NCH):
            deps = (fin[j - 2][0],) if j >= 2 else ()
            keep_d, keep_u, send = chunk_grads(j, tab, info, srcs, wus, wds, deps)
            recv = x_swap(send)
            *outs, fd, fuc, fus = finish(j, pos, keep_d, keep_u, recv, outs)
            rd = y_swap(fd)
            ruc = y_swap(fuc)
            ruy = y_diag(fus)
            rus = core_swap(fus)
            fin.append((fd, (rd, ruc, ruy, rus)))
            if j >= 2:
                outs = store(j - 2, pos, *fin[j - 2][1], outs)
        for j in range(NCH - 2, NCH):
            outs = store(j, pos, *fin[j][1], outs)
        return outs[1][None], outs[0][None]

    return jax.shard_map(
        group_grads,
        mesh=mesh,
        in_specs=(tok_spec, tok_spec, len_spec, w_spec, w_spec),
        out_specs=(w_spec, w_spec),
        check_vma=False,
    )
```

```python
import jax
import jax.numpy as jnp
from jax import lax
from jax.experimental import pallas as pl
from jax.experimental.pallas import tpu as pltpu
from jax.sharding import PartitionSpec as P


D = 2048
TOK = 1024
MICRO = 3
BASE = 256
REST = TOK - BASE
TM = 128
NT = MICRO * REST // TM
RROWS = MICRO * REST + TM
FIRST = 3
CAPS = (6, 6, 3)
G = 4
M = G * TM
FB = 256
HB = FB // 2
NCH = D // FB
HALF = 1024
WH = 512
C1 = 0.7978845608028654
C3 = 0.044715
BF = jnp.bfloat16
F32 = jnp.float32


ANY = pl.BlockSpec(memory_space=pl.ANY)
SM = pl.BlockSpec(memory_space=pltpu.SMEM)
VM = pl.BlockSpec(memory_space=pltpu.VMEM)
MIB = 1024 * 1024

CORE = [(0, 1), (1, 0), (2, 3), (3, 2)]
XSWAP = [(0, 2), (2, 0), (1, 3), (3, 1)]
XDIAG = [(0, 3), (3, 0), (1, 2), (2, 1)]
YSWAP = [(0, 1), (1, 0)]
YDIAG = [(r * 4 + f, (1 - r) * 4 + (f ^ 1)) for r in range(2) for f in range(4)]


def core_swap(v):
    return lax.ppermute(v, "fsdp", CORE)


def x_swap(v):
    return lax.ppermute(v, "fsdp", XSWAP)


def x_diag(v):
    return lax.ppermute(v, "fsdp", XDIAG)


def y_swap(v):
    return lax.ppermute(v, "replica", YSWAP)


def y_diag(v):
    return lax.ppermute(v, ("replica", "fsdp"), YDIAG)


def cost(flops, nbytes):
    return pl.CostEstimate(flops=flops, bytes_accessed=nbytes, transcendentals=0)


def pack_rest(x_in, dy, rest, offs):
    def kern(rest_ref, offs_ref, x_ref, d_ref, out_ref, buf, zero, isem, osem, zsem):
        loads = []
        for k in range(MICRO):
            for a, ref in enumerate((x_ref, d_ref)):
                cp = pltpu.make_async_copy(ref.at[k, pl.ds(BASE, REST), :], buf.at[k, a], isem.at[k, a])
                cp.start()
                loads.append(cp)
        zero[...] = jnp.zeros_like(zero)
        for k in range(MICRO):
            n = rest_ref[k]
            for a in range(2):
                loads[2 * k + a].wait()
                for r in range(0, REST, TM):
                    row = lax.broadcasted_iota(jnp.int32, (TM, D), 0) + r
                    blk = buf[k, a, r : r + TM, :]
                    buf[k, a, r : r + TM, :] = jnp.where(row < n, blk, jnp.zeros_like(blk))
            o = pl.multiple_of(offs_ref[k], 16)
            cps = [
                pltpu.make_async_copy(buf.at[k, a], out_ref.at[a, pl.ds(o, REST), :], osem.at[a]) for a in range(2)
            ]
            for cp in cps:
                cp.start()
            for cp in cps:
                cp.wait()
        for o in (pl.multiple_of(offs_ref[MICRO], 16), MICRO * REST):
            cps = [pltpu.make_async_copy(zero, out_ref.at[a, pl.ds(o, TM), :], zsem.at[a]) for a in range(2)]
            for cp in cps:
                cp.start()
            for cp in cps:
                cp.wait()

    return pl.pallas_call(
        kern,
        in_specs=[SM, SM, ANY, ANY],
        out_specs=ANY,
        out_shape=jax.ShapeDtypeStruct((2, RROWS, D), BF),
        scratch_shapes=[
            pltpu.VMEM((MICRO, 2, REST, D), BF),
            pltpu.VMEM((TM, D), BF),
            pltpu.SemaphoreType.DMA((MICRO, 2)),
            pltpu.SemaphoreType.DMA((2,)),
            pltpu.SemaphoreType.DMA((2,)),
        ],
        compiler_params=pltpu.CompilerParams(vmem_limit_bytes=40 * MIB),
        cost_estimate=cost(15_000_000_000, 50_000_000),
        name="pack_rest",
    )(rest, offs, x_in, dy)


def build_send(own, sib, info):
    def kern(info_ref, own_ref, sib_ref, *refs):
        outs, (buf, isem, osem) = refs[:4], refs[4:]
        n, mine, shift = info_ref[0], info_ref[1], info_ref[2]
        starts = (0, FIRST, info_ref[3], info_ref[4])

        def load(i, slot):
            @pl.when(i < mine)
            def _():
                r = pl.multiple_of(i * TM, TM)
                pltpu.make_async_copy(own_ref.at[:, pl.ds(r, TM), :], buf.at[slot], isem.at[slot]).start()

            @pl.when(i >= mine)
            def _():
                r = pl.multiple_of((i + shift) * TM, TM)
                pltpu.make_async_copy(sib_ref.at[:, pl.ds(r, TM), :], buf.at[slot], isem.at[slot]).start()

        def store(i, slot):
            for k in range(4):
                here = i >= starts[k]
                if k < 3:
                    here = jnp.logical_and(here, i < starts[k + 1])

                @pl.when(here)
                def _():
                    r = pl.multiple_of((i - starts[k]) * TM, TM)
                    pltpu.make_async_copy(buf.at[slot], outs[k].at[:, pl.ds(r, TM), :], osem.at[slot]).start()

        def stored(slot):
            pltpu.make_async_copy(buf.at[slot], outs[0].at[:, pl.ds(0, TM), :], osem.at[slot]).wait()

        for s in range(3):

            @pl.when(s < n)
            def _():
                load(s, s)

        def body(i, _):
            slot = lax.rem(i, 4)
            pltpu.make_async_copy(own_ref.at[:, pl.ds(0, TM), :], buf.at[slot], isem.at[slot]).wait()
            store(i, slot)

            @pl.when(i >= 1)
            def _():
                stored(lax.rem(i + 3, 4))

            @pl.when(i + 3 < n)
            def _():
                load(i + 3, lax.rem(i + 3, 4))

            return 0

        lax.fori_loop(0, n, body, 0)

        @pl.when(n > 0)
        def _():
            stored(lax.rem(n + 3, 4))

    return pl.pallas_call(
        kern,
        in_specs=[SM, ANY, ANY],
        out_specs=[ANY] * 4,
        out_shape=[jax.ShapeDtypeStruct((2, k * TM, D), BF) for k in (FIRST, *CAPS)],
        scratch_shapes=[pltpu.VMEM((4, 2, TM, D), BF), pltpu.SemaphoreType.DMA((4,)), pltpu.SemaphoreType.DMA((4,))],
        cost_estimate=cost(10_000_000_000, 36_000_000),
        name="build_send",
    )(info, own, sib)


def gelu_and_slope(u):
    u2 = u * u
    t = jnp.tanh(u * (C1 + (C1 * C3) * u2))
    half = 0.5 + 0.5 * t
    act = u * half
    slope = half + (0.5 * u) * (1.0 - t * t) * (C1 + (3 * C1 * C3) * u2)
    return act, slope


def pick(e, lo, hi, fn):
    if hi - lo == 1:
        fn(lo)
        return
    mid = (lo + hi) // 2

    @pl.when(e < mid * 32)
    def _():
        pick(e, lo, mid, fn)

    @pl.when(e >= mid * 32)
    def _():
        pick(e, mid, hi, fn)


def issue_group(tab_ref, g, slot, src, xb, db, sem):
    for s in range(G):
        e = tab_ref[g * G + s]
        r = pl.multiple_of(lax.rem(e, 32) * TM, TM)

        def fetch(k):
            rows = pl.ds(s * TM, TM)
            pltpu.make_async_copy(src[k].at[0, pl.ds(r, TM), :], xb.at[slot, rows, :], sem.at[slot, 0]).start()
            pltpu.make_async_copy(src[k].at[1, pl.ds(r, TM), :], db.at[slot, rows, :], sem.at[slot, 1]).start()

        pick(e, 0, len(src), fetch)


def wait_group(slot, xb, db, sem):
    pltpu.make_async_copy(xb.at[slot], xb.at[slot], sem.at[slot, 0]).wait()
    pltpu.make_async_copy(db.at[slot], db.at[slot], sem.at[slot, 1]).wait()


def add_group(x, dy, wu, wd, gd, gu):
    u = jnp.dot(x, wu[...], preferred_element_type=F32).astype(BF).astype(F32)
    da = lax.dot_general(dy, wd[...], (((1,), (1,)), ((), ())), preferred_element_type=F32)
    act, slope = gelu_and_slope(u)
    dh = (da * slope).astype(BF)
    gd[...] += lax.dot_general(act.astype(BF), dy, (((0,), (0,)), ((), ())), preferred_element_type=F32)
    gu[...] += lax.dot_general(dh, x, (((0,), (0,)), ((), ())), preferred_element_type=F32)


def weight_copies(c, f, w, wub, wdb, sem):
    own, sib, fx, fd, wd_own, wd_oth = w
    cps = []
    c0 = c * HB
    co = (c % (WH // HB)) * HB
    if not isinstance(c, int):
        c0, co = pl.multiple_of(c0, HB), pl.multiple_of(co, HB)
    for a in range(2):
        for k, (ref, col) in enumerate(((own, c0), (sib, c0), (fx, co), (fd, co))):
            rows = pl.ds(pl.multiple_of((f ^ k) * 512, 512), 512)
            cps.append(
                pltpu.make_async_copy(
                    ref.at[a, :, pl.ds(col, HB)], wub.at[rows, pl.ds(a * HB, HB)], sem.at[k, a]
                )
            )
    cps.append(pltpu.make_async_copy(wd_own.at[pl.ds(c0, HB), :], wdb.at[pl.ds(0, HB), :], sem.at[4, 0]))
    cps.append(pltpu.make_async_copy(wd_oth.at[pl.ds(co, HB), :], wdb.at[pl.ds(HB, HB), :], sem.at[4, 1]))
    return cps


def gather_scratch(n_acc):
    return [
        pltpu.VMEM((2, M, D), BF),
        pltpu.VMEM((2, M, D), BF),
        pltpu.VMEM((n_acc, D, FB), BF),
        pltpu.VMEM((n_acc, FB, D), BF),
        pltpu.VMEM((n_acc, FB, D), F32),
        pltpu.VMEM((n_acc, FB, D), F32),
        pltpu.SemaphoreType.DMA((2, 2)),
        pltpu.SemaphoreType.DMA((n_acc, 5, 2)),
    ]


def early_grads(tab, info, srcs, wsets, lo_chunk, n_chunks, prior, flops):
    ns, nw, npr = len(srcs), len(wsets), len(prior)
    per = WH // HB

    def kern(tab_ref, info_ref, *refs):
        src, refs = refs[:ns], refs[ns:]
        wset = [refs[6 * k : 6 * k + 6] for k in range(nw)]
        refs = refs[6 * nw :]
        pri, refs = refs[: 2 * npr], refs[2 * npr :]
        out_d, out_u, xb, db, wub, wdb, gd, gu, sem, wsem, asem = refs
        f = info_ref[3]
        done_before = sum(p[0].shape[0] for p in prior)

        def lo(q):
            return jnp.where(q < done_before, info_ref[0], 0)

        hi = info_ref[1]

        def weights(q, slot, act):
            c = lo_chunk + q
            for k in range(nw):
                here = c // per == (lo_chunk // per) + k

                @pl.when(here)
                def _():
                    for cp in weight_copies(c, f, wset[k], wub.at[slot], wdb.at[slot], wsem.at[slot]):
                        act(cp)

        def start(cp):
            cp.start()

        def wait(cp):
            cp.wait()

        def results(q, slot):
            return (
                pltpu.make_async_copy(gd.at[slot], out_d.at[q], asem.at[slot, 0]),
                pltpu.make_async_copy(gu.at[slot], out_u.at[q], asem.at[slot, 1]),
            )

        issue_group(tab_ref, lo(0), 0, src, xb, db, sem)
        weights(0, 0, start)

        def chunk(q, t):
            ws = lax.rem(q, 2)

            @pl.when(q + 1 < n_chunks)
            def _():
                weights(q + 1, 1 - ws, start)

            @pl.when(q >= 2)
            def _():
                for cp in results(q - 2, ws):
                    cp.wait()

            base = 0
            for k in range(npr):
                size = prior[k][0].shape[0]
                lo_q, hi_q = base, base + size
                base = hi_q

                @pl.when(jnp.logical_and(q >= lo_q, q < hi_q))
                def _():
                    cps = (
                        pltpu.make_async_copy(pri[2 * k].at[q - lo_q], gd.at[ws], asem.at[ws, 0]),
                        pltpu.make_async_copy(pri[2 * k + 1].at[q - lo_q], gu.at[ws], asem.at[ws, 1]),
                    )
                    for cp in cps:
                        cp.start()
                    for cp in cps:
                        cp.wait()

            @pl.when(q >= base)
            def _():
                gd[ws] = jnp.zeros((FB, D), F32)
                gu[ws] = jnp.zeros((FB, D), F32)

            weights(q, ws, wait)

            def group(g, t):
                slot = lax.rem(t, 2)
                last = g + 1 == hi
                nxt = jnp.where(last, lo(q + 1), g + 1)

                @pl.when(jnp.logical_or(jnp.logical_not(last), q + 1 < n_chunks))
                def _():
                    issue_group(tab_ref, nxt, 1 - slot, src, xb, db, sem)

                wait_group(slot, xb, db, sem)
                add_group(xb[slot], db[slot], wub.at[ws], wdb.at[ws], gd.at[ws], gu.at[ws])
                return t + 1

            t = lax.fori_loop(lo(q), hi, group, t)
            for cp in results(q, ws):
                cp.start()
            return t

        lax.fori_loop(0, n_chunks, chunk, 0)
        for q in range(max(n_chunks - 2, 0), n_chunks):
            for cp in results(q, q % 2):
                cp.wait()

    flat = [w for ws in wsets for w in ws]
    pri = [a for p in prior for a in p]
    return pl.pallas_call(
        kern,
        in_specs=[SM, SM] + [ANY] * (ns + len(flat) + len(pri)),
        out_specs=[ANY] * 2,
        out_shape=[jax.ShapeDtypeStruct((n_chunks, FB, D), F32)] * 2,
        scratch_shapes=gather_scratch(2) + [pltpu.SemaphoreType.DMA((2, 2))],
        compiler_params=pltpu.CompilerParams(vmem_limit_bytes=48 * MIB),
        cost_estimate=cost(flops, 200_000_000),
    )(tab, info, *srcs, *flat, *pri)


def chunk_grads(j, tab, info, srcs, w, prior, deps):
    ns = len(srcs)

    def kern(tab_ref, info_ref, *refs):
        src, refs = refs[:ns], refs[ns:]
        wrefs, (pd, pu), refs = refs[:6], refs[6:8], refs[8 + len(deps) :]
        keep_d, keep_u, send_d, send_u, xb, db, wub, wdb, gd, gu, sem, wsem, osem = refs
        groups, xi, f = info_ref[0], info_ref[1], info_ref[2]
        wub, wdb, gd, gu = wub.at[0], wdb.at[0], gd.at[0], gu.at[0]
        cps = weight_copies(j, f, wrefs, wub, wdb, wsem.at[0])
        cps.append(pltpu.make_async_copy(pd.at[j], gd, osem.at[0]))
        cps.append(pltpu.make_async_copy(pu.at[j], gu, osem.at[1]))
        for cp in cps:
            cp.start()

        @pl.when(groups > 0)
        def _():
            issue_group(tab_ref, 0, 0, src, xb, db, sem)

        for cp in cps:
            cp.wait()

        def body(g, _):
            slot = lax.rem(g, 2)

            @pl.when(g + 1 < groups)
            def _():
                issue_group(tab_ref, g + 1, 1 - slot, src, xb, db, sem)

            wait_group(slot, xb, db, sem)
            add_group(xb[slot], db[slot], wub, wdb, gd, gu)
            return 0

        lax.fori_loop(0, groups, body, 0)
        kc = pl.multiple_of(xi * HALF, HALF)
        sc = pl.multiple_of((1 - xi) * HALF, HALF)
        ocp = [
            (gd.at[pl.ds(HB, HB), :], send_d),
            (gu.at[pl.ds(0, HB), pl.ds(sc, HALF)], send_u.at[:, pl.ds(0, HALF)]),
            (gu.at[pl.ds(HB, HB), pl.ds(sc, HALF)], send_u.at[:, pl.ds(HALF, HALF)]),
            (gd.at[pl.ds(0, HB), :], keep_d),
            (gu.at[:, pl.ds(kc, HALF)], keep_u),
        ]
        ocp = [pltpu.make_async_copy(a, b, osem.at[i]) for i, (a, b) in enumerate(ocp)]
        for cp in ocp:
            cp.start()
        for cp in ocp:
            cp.wait()

    n_in = ns + 8 + len(deps)
    return pl.pallas_call(
        kern,
        in_specs=[SM, SM] + [ANY] * n_in,
        out_specs=[ANY] * 4,
        out_shape=[
            jax.ShapeDtypeStruct((HB, D), F32),
            jax.ShapeDtypeStruct((FB, HALF), F32),
            jax.ShapeDtypeStruct((HB, D), F32),
            jax.ShapeDtypeStruct((HB, D), F32),
        ],
        scratch_shapes=gather_scratch(1) + [pltpu.SemaphoreType.DMA((5,))],
        compiler_params=pltpu.CompilerParams(vmem_limit_bytes=40 * MIB),
        cost_estimate=cost(8 * 3072 * D * FB, 40_000_000),
    )(tab, info, *srcs, *w, *prior, *deps)


def finish_down(j, pos, keep, recv, out):
    first = out is None

    def kern(pos_ref, kd, rc, *refs):
        out_d, fd, vd, sem = refs if first else refs[1:]
        y = pos_ref[0]
        vd[...] = kd[...] + rc[...]
        row = pl.multiple_of(y * HALF + j * HB, HB)
        cps = [
            pltpu.make_async_copy(vd, fd, sem.at[0]),
            pltpu.make_async_copy(vd, out_d.at[pl.ds(row, HB), :], sem.at[1]),
        ]
        for cp in cps:
            cp.start()
        for cp in cps:
            cp.wait()

    extra = [] if first else [out]
    return pl.pallas_call(
        kern,
        in_specs=[SM, VM, VM] + [ANY] * len(extra),
        out_specs=[ANY] * 2,
        out_shape=[jax.ShapeDtypeStruct((D, D), F32), jax.ShapeDtypeStruct((HB, D), F32)],
        scratch_shapes=[pltpu.VMEM((HB, D), F32), pltpu.SemaphoreType.DMA((2,))],
        input_output_aliases={} if first else {3: 0},
        compiler_params=pltpu.CompilerParams(vmem_limit_bytes=16 * MIB),
        cost_estimate=cost(2_000_000_000, 4_000_000),
    )(pos, keep, recv, *extra)


def finish_up(j, pos, keep, recv, out):
    first = out is None

    def kern(pos_ref, ku, rc, *refs):
        out_u, fuc, fus, vu, sem = refs if first else refs[1:]
        y, xi, c = pos_ref[0], pos_ref[1], pos_ref[2]
        mine = pl.ds(pl.multiple_of(c * 512, 512), 512)
        other = pl.ds(pl.multiple_of((1 - c) * 512, 512), 512)
        vu[0] = (ku[0:HB, :] + rc[:, HALF:D]).T
        vu[1] = (ku[HB:FB, :] + rc[:, 0:HALF]).T
        cps = [
            pltpu.make_async_copy(vu.at[:, other, :], fus, sem.at[0]),
            pltpu.make_async_copy(vu.at[:, mine, :], fuc, sem.at[1]),
        ]
        for a in range(2):
            xa = xi if a == 0 else 1 - xi
            col = pl.multiple_of(((2 * xa + c) * 2 + y) * HALF + j * HB, HB)
            cps.append(pltpu.make_async_copy(vu.at[a, mine, :], out_u.at[:, pl.ds(col, HB)], sem.at[2 + a]))
        for cp in cps:
            cp.start()
        for cp in cps:
            cp.wait()

    extra = [] if first else [out]
    return pl.pallas_call(
        kern,
        in_specs=[SM, VM, VM] + [ANY] * len(extra),
        out_specs=[ANY] * 3,
        out_shape=[
            jax.ShapeDtypeStruct((512, 4 * D), F32),
            jax.ShapeDtypeStruct((2, 512, HB), F32),
            jax.ShapeDtypeStruct((2, 512, HB), F32),
        ],
        scratch_shapes=[pltpu.VMEM((2, HALF, HB), F32), pltpu.SemaphoreType.DMA((4,))],
        input_output_aliases={} if first else {3: 0},
        compiler_params=pltpu.CompilerParams(vmem_limit_bytes=16 * MIB),
        cost_estimate=cost(2_000_000_000, 4_000_000),
    )(pos, keep, recv, *extra)


def store(j, pos, rd, ruc, ruy, rus, outs):
    def kern(pos_ref, d_ref, uc_ref, uy_ref, us_ref, _d, _u, out_d, out_u, vd, vu, isem, osem):
        y, xi, c = pos_ref[0], pos_ref[1], pos_ref[2]
        loads = [pltpu.make_async_copy(d_ref, vd, isem.at[0])]
        for k, r in enumerate((uc_ref, uy_ref, us_ref)):
            loads.append(pltpu.make_async_copy(r, vu.at[k], isem.at[1 + k]))
        for cp in loads:
            cp.start()
        row = pl.multiple_of((1 - y) * HALF + j * HB, HB)
        loads[0].wait()
        outc = [pltpu.make_async_copy(vd, out_d.at[pl.ds(row, HB), :], osem.at[0])]
        outc[0].start()
        for k, (cc, yy) in enumerate(((c, 1 - y), (1 - c, 1 - y), (1 - c, y))):
            loads[1 + k].wait()
            for a in range(2):
                xa = xi if a == 0 else 1 - xi
                col = pl.multiple_of(((2 * xa + cc) * 2 + yy) * HALF + j * HB, HB)
                cp = pltpu.make_async_copy(vu.at[k, a], out_u.at[:, pl.ds(col, HB)], osem.at[1 + 2 * k + a])
                cp.start()
                outc.append(cp)
        for cp in outc:
            cp.wait()

    return pl.pallas_call(
        kern,
        in_specs=[SM] + [ANY] * 6,
        out_specs=[ANY] * 2,
        out_shape=[jax.ShapeDtypeStruct((D, D), F32), jax.ShapeDtypeStruct((512, 4 * D), F32)],
        scratch_shapes=[
            pltpu.VMEM((HB, D), F32),
            pltpu.VMEM((3, 2, 512, HB), F32),
            pltpu.SemaphoreType.DMA((4,)),
            pltpu.SemaphoreType.DMA((7,)),
        ],
        input_output_aliases={5: 0, 6: 1},
        compiler_params=pltpu.CompilerParams(vmem_limit_bytes=16 * MIB),
        cost_estimate=cost(3_000_000_000, 5_000_000),
    )(pos, rd, ruc, ruy, rus, *outs)


def exchange_branch(n):
    last = min(n, CAPS[2])
    full = CAPS[1] if n - last > CAPS[0] else 0
    part = n - last - full

    def swapped(piece, k, cap):
        if k == 0:
            return jnp.zeros((2, cap * TM, D), BF)
        return y_swap(piece if k == cap else piece[:, : k * TM])

    def padded(v, cap):
        short = cap * TM - v.shape[1]
        return lax.pad(v, jnp.zeros((), BF), ((0, 0, 0), (0, short, 0), (0, 0, 0))) if short else v

    def run(p0, p1, p2, early):
        g1 = swapped(p1, full, CAPS[1])
        g0 = swapped(p0, part, CAPS[0])
        g2 = swapped(p2, last, CAPS[2])
        acc = early()
        s1 = core_swap(g1) if full else g1
        s0 = core_swap(g0) if part else g0
        return (padded(g0, CAPS[0]), g1, padded(g2, CAPS[2]), padded(s0, CAPS[0]), s1, *acc)

    return run


def solution(mesh):
    tok_spec = P(None, ("model", "replica", "fsdp"), None)
    len_spec = P(None, ("model", "replica", "fsdp"))
    w_spec = P(None, ("model", "fsdp"), None)

    def group_grads(x_in, dy, lengths, w_up, w_down):
        y, f = lax.axis_index("replica"), lax.axis_index("fsdp")
        xi, c = f // 2, f % 2
        w_up, w_down = w_up[0], w_down[0]

        lens = lax.all_gather(lengths[:, 0], ("replica", "fsdp")).astype(jnp.int32)

        s1 = jnp.stack([x_in[:, :BASE], dy[:, :BASE]]).reshape(2, MICRO * BASE, D)

        def cols(xd, cd, lo=0, n=HALF):
            own = lax.dynamic_slice(w_up, (0, ((2 * xd + cd) * 2 + y) * HALF + lo), (512, n))
            oth = lax.dynamic_slice(w_up, (0, ((2 * (1 - xd) + cd) * 2 + y) * HALF + lo), (512, n))
            return jnp.stack([own, oth])

        wd_own = lax.dynamic_slice(w_down, (y * HALF, 0), (HALF, D))
        to_x = [cols(1 - xi, c, lo, WH) for lo in (0, WH)]
        to_d = [cols(1 - xi, 1 - c, lo, WH) for lo in (0, WH)]
        wd_h = [wd_own[lo : lo + WH] for lo in (0, WH)]
        (lens, s1, to_x, to_d, wd_h) = lax.optimization_barrier((lens, s1, to_x, to_d, wd_h))
        s1_y = y_swap(s1)
        wx = []
        for h in range(2):
            a = x_swap(to_x[h])
            b = x_diag(to_d[h])
            d = x_swap(wd_h[h])
            wx.append((a, b, d))
        from_s = core_swap(cols(xi, 1 - c))
        mine = cols(xi, c)
        wsets = [(mine, from_s, a, b, wd_own, d) for a, b, d in wx]

        rest = lens - BASE
        r16 = (rest + 15) // 16 * 16
        tiles = (jnp.sum(r16, axis=1) + TM - 1) // TM
        me = y * 4 + f
        my_rest = lax.dynamic_index_in_dim(rest, me, keepdims=False)
        my16 = lax.dynamic_index_in_dim(r16, me, keepdims=False)
        offs = jnp.concatenate([jnp.zeros((1,), jnp.int32), jnp.cumsum(my16)])
        both = tiles[0::2] + tiles[1::2]
        share = jnp.stack([(both + 1) // 2, both // 2], axis=1).reshape(8)
        more = jnp.maximum(jnp.max(share) - FIRST, 0)

        def at(v, i):
            return lax.dynamic_index_in_dim(v, i, keepdims=False)

        t_own, t_sib = at(tiles, me), at(tiles, me ^ 1)
        h_own = at(share, me)
        h_y, h_ys = at(share, me ^ 4), at(share, me ^ 5)
        left = jnp.maximum(more - CAPS[2], 0)
        full = jnp.where(left > CAPS[0], CAPS[1], 0)
        at1 = FIRST + left - full
        at2 = at1 + full

        packed = pack_rest(x_in, dy, my_rest, offs)
        packed_s = core_swap(packed)
        s1_s = core_swap(s1)
        pa, p0, p1, p2 = build_send(
            packed, packed_s, jnp.stack([h_own, t_own, t_sib - h_own, at1, at2]).astype(jnp.int32)
        )
        qa = y_swap(pa)

        i = jnp.arange(64)
        n_own = 12 + t_own + t_sib
        g_own = (n_own + G - 1) // G
        k = i - g_own * G
        tab = jnp.where(i < n_own, 3 * 32 + i - 12 - t_own, 2 * 32 + NT)
        tab = jnp.where(i < 12 + t_own, 2 * 32 + i - 12, tab)
        tab = jnp.where(i < 12, (i // 6) * 32 + i % 6, tab)
        tab = jnp.where((k >= 0) & (k < 12), (4 + k // 6) * 32 + k % 6, tab).astype(jnp.int32)
        info_own = jnp.stack([0, g_own, xi, f]).astype(jnp.int32)
        info_all = jnp.stack([g_own, g_own + 3, xi, f]).astype(jnp.int32)

        i = jnp.arange(40)
        own_list = i < h_y
        t = jnp.where(own_list, i, i - h_y)
        s = jnp.where(t < FIRST, t, jnp.where(t < at1, 32 + t - FIRST, jnp.where(t < at2, 64 + t - at1, 96 + t - at2)))
        late = jnp.where(own_list, s, s + 128)
        late = jnp.where(i < h_y + h_ys, late, 256 + NT).astype(jnp.int32)
        info_late = jnp.stack([(h_y + h_ys + G - 1) // G, xi, f]).astype(jnp.int32)
        pos = jnp.stack([y, xi, c]).astype(jnp.int32)

        own_srcs = (s1, s1_s, packed, packed_s)
        acc0 = early_grads(tab, info_own, own_srcs, wsets[:1], 0, 2, [], 8 * 4096 * D * FB * 2)
        s1_ys = core_swap(s1_y)
        acc1 = early_grads(tab, info_own, own_srcs, wsets[:1], 2, 2, [], 8 * 4096 * D * FB * 2)

        def branch(n):
            run = exchange_branch(n)

            def go(p0, p1, p2, tab, info, srcs, wsets, acc0, acc1):
                return run(
                    p0, p1, p2,
                    lambda: early_grads(tab, info, srcs, wsets, 0, NCH, [acc0, acc1], 8 * 4096 * D * FB * 5),
                )

            return go

        srcs = (*own_srcs, s1_y, s1_ys)
        q0, q1, q2, q0s, q1s, accd, accu = lax.switch(
            more, [branch(n) for n in range(NT - FIRST + 1)],
            p0, p1, p2, tab, info_all, srcs, [list(w) for w in wsets], list(acc0), list(acc1),
        )
        qas = core_swap(qa)
        q2s = core_swap(q2)
        srcs = (qa, q0, q1, q2, qas, q0s, q1s, q2s, packed)

        out_d = out_u = None
        fin = []
        for j in range(NCH):
            deps = (fin[j - 2][0],) if j >= 2 else ()
            keep_d, keep_u, send_d, send_u = chunk_grads(
                j, late, info_late, srcs, wsets[j * HB // WH], (accd, accu), deps
            )
            recv_d = x_swap(send_d)
            recv_u = x_swap(send_u)
            out_d, fd = finish_down(j, pos, keep_d, recv_d, out_d)
            out_u, fuc, fus = finish_up(j, pos, keep_u, recv_u, out_u)
            rd = y_swap(fd)
            ruc = y_swap(fuc)
            ruy = y_diag(fus)
            rus = core_swap(fus)
            fin.append((fuc, (rd, ruc, ruy, rus)))
            if j >= 2:
                out_d, out_u = store(j - 2, pos, *fin[j - 2][1], (out_d, out_u))
        for j in range(NCH - 2, NCH):
            out_d, out_u = store(j, pos, *fin[j][1], (out_d, out_u))
        return out_u[None], out_d[None]

    return jax.shard_map(
        group_grads,
        mesh=mesh,
        in_specs=(tok_spec, tok_spec, len_spec, w_spec, w_spec),
        out_specs=(w_spec, w_spec),
        check_vma=False,
    )
```

```python
import jax
import jax.numpy as jnp
from jax import lax
from jax.experimental import pallas as pl
from jax.experimental.pallas import tpu as pltpu
from jax.sharding import PartitionSpec as P


D = 2048
TOK = 1024
MICRO = 3
BASE = 256
REST = TOK - BASE
TM = 128
NT = MICRO * REST // TM
RROWS = MICRO * REST + TM
FIRST = 3
PIECES = (4, 4, 4, 2, 1)
SIZES = (5, 7, 8, 9, 10, 11, 12, 15)
G = 4
M = G * TM
FB = 256
HB = FB // 2
NCH = D // FB
HALF = 1024
WSETS = ((0, 2), (2, 2), (4, 4))
ORDER = (3, 4, 0, 5, 6, 1, 7, 2)
LAG = 3
OWN_ONLY = 3
C1 = 0.7978845608028654
C3 = 0.044715
BF = jnp.bfloat16
F32 = jnp.float32


ANY = pl.BlockSpec(memory_space=pltpu.HBM)
SM = pl.BlockSpec(memory_space=pltpu.SMEM)
VM = pl.BlockSpec(memory_space=pltpu.VMEM)
MIB = 1024 * 1024
GRANT = 60 * 1024 * 1024

CORE = [(0, 1), (1, 0), (2, 3), (3, 2)]
XSWAP = [(0, 2), (2, 0), (1, 3), (3, 1)]
XDIAG = [(0, 3), (3, 0), (1, 2), (2, 1)]
YSWAP = [(0, 1), (1, 0)]
YDIAG = [(r * 4 + f, (1 - r) * 4 + (f ^ 1)) for r in range(2) for f in range(4)]


def core_swap(v):
    return lax.ppermute(v, "fsdp", CORE)


def x_swap(v):
    return lax.ppermute(v, "fsdp", XSWAP)


def x_diag(v):
    return lax.ppermute(v, "fsdp", XDIAG)


def y_swap(v):
    return lax.ppermute(v, "replica", YSWAP)


def y_diag(v):
    return lax.ppermute(v, ("replica", "fsdp"), YDIAG)


def cost(flops, nbytes):
    return pl.CostEstimate(flops=flops, bytes_accessed=nbytes, transcendentals=0)


def start(lens, x_in, dy):
    def kern(len_ref, x_ref, d_ref, all_ref, s1_ref, land, buf, send, recv, isem, osem):
        r, f = lax.axis_index("replica"), lax.axis_index("fsdp")
        me = r * 4 + f
        loads = []
        for a, ref in enumerate((x_ref, d_ref)):
            cp = pltpu.make_async_copy(ref.at[:, pl.ds(0, BASE), :], buf.at[a], isem.at[a])
            cp.start()
            loads.append(cp)
        barrier = pltpu.get_barrier_semaphore()
        peers = []
        for k in range(1, 8):
            p = lax.rem(me + k, 8)
            peers.append((0, p // 4, lax.rem(p, 4)))
        for p in peers:
            pl.semaphore_signal(barrier, inc=1, device_id=p, device_id_type=pl.DeviceIdType.MESH)
        pl.semaphore_wait(barrier, 7)
        cps = []
        for k, p in enumerate(peers):
            cp = pltpu.make_async_remote_copy(
                src_ref=len_ref,
                dst_ref=land.at[k],
                send_sem=send.at[k],
                recv_sem=recv.at[k],
                device_id=p,
                device_id_type=pl.DeviceIdType.MESH,
            )
            cp.start()
            cps.append(cp)
        outs = []
        for a in range(2):
            loads[a].wait()
            cp = pltpu.make_async_copy(buf.at[a], s1_ref.at[a], osem.at[a])
            cp.start()
            outs.append(cp)
        for cp in cps:
            cp.wait()
        all_ref[0] = len_ref[...]
        for k in range(7):
            all_ref[k + 1] = land[k]
        for cp in outs:
            cp.wait()

    return pl.pallas_call(
        kern,
        in_specs=[VM, ANY, ANY],
        out_specs=[VM, ANY],
        out_shape=[jax.ShapeDtypeStruct((8, 8, 128), jnp.int32), jax.ShapeDtypeStruct((2, MICRO, BASE, D), BF)],
        scratch_shapes=[
            pltpu.VMEM((7, 8, 128), jnp.int32),
            pltpu.VMEM((2, MICRO, BASE, D), BF),
            pltpu.SemaphoreType.DMA((7,)),
            pltpu.SemaphoreType.DMA((7,)),
            pltpu.SemaphoreType.DMA((2,)),
            pltpu.SemaphoreType.DMA((2,)),
        ],
        compiler_params=pltpu.CompilerParams(collective_id=0, has_side_effects=True, vmem_limit_bytes=GRANT),
        cost_estimate=cost(10_000_000_000, 13_000_000),
        name="start",
    )(lens, x_in, dy)


def pack_rest(x_in, dy, rest, offs):
    def kern(rest_ref, offs_ref, x_ref, d_ref, out_ref, buf, zero, isem, osem, zsem):
        loads = []
        for k in range(MICRO):
            for a, ref in enumerate((x_ref, d_ref)):
                cp = pltpu.make_async_copy(ref.at[k, pl.ds(BASE, REST), :], buf.at[k, a], isem.at[k, a])
                cp.start()
                loads.append(cp)
        zero[...] = jnp.zeros_like(zero)
        for k in range(MICRO):
            n = rest_ref[k]
            for a in range(2):
                loads[2 * k + a].wait()
                for r in range(0, REST, TM):
                    row = lax.broadcasted_iota(jnp.int32, (TM, D), 0) + r
                    blk = buf[k, a, r : r + TM, :]
                    buf[k, a, r : r + TM, :] = jnp.where(row < n, blk, jnp.zeros_like(blk))
            o = pl.multiple_of(offs_ref[k], 16)
            cps = [
                pltpu.make_async_copy(buf.at[k, a], out_ref.at[a, pl.ds(o, REST), :], osem.at[a]) for a in range(2)
            ]
            for cp in cps:
                cp.start()
            for cp in cps:
                cp.wait()
        for o in (pl.multiple_of(offs_ref[MICRO], 16), MICRO * REST):
            cps = [pltpu.make_async_copy(zero, out_ref.at[a, pl.ds(o, TM), :], zsem.at[a]) for a in range(2)]
            for cp in cps:
                cp.start()
            for cp in cps:
                cp.wait()

    return pl.pallas_call(
        kern,
        in_specs=[SM, SM, ANY, ANY],
        out_specs=ANY,
        out_shape=jax.ShapeDtypeStruct((2, RROWS, D), BF),
        scratch_shapes=[
            pltpu.VMEM((MICRO, 2, REST, D), BF),
            pltpu.VMEM((TM, D), BF),
            pltpu.SemaphoreType.DMA((MICRO, 2)),
            pltpu.SemaphoreType.DMA((2,)),
            pltpu.SemaphoreType.DMA((2,)),
        ],
        compiler_params=pltpu.CompilerParams(vmem_limit_bytes=GRANT),
        cost_estimate=cost(15_000_000_000, 50_000_000),
        name="pack_rest",
    )(rest, offs, x_in, dy)


def build_send(own, sib, info):
    np_ = 1 + len(PIECES)

    def kern(info_ref, own_ref, sib_ref, *refs):
        outs, (buf, isem, osem) = refs[:np_], refs[np_:]
        n, mine, shift = info_ref[0], info_ref[1], info_ref[2]
        starts = [0] + [info_ref[3 + k] for k in range(len(PIECES))]

        def load(i, slot):
            @pl.when(i < mine)
            def _():
                r = pl.multiple_of(i * TM, TM)
                pltpu.make_async_copy(own_ref.at[:, pl.ds(r, TM), :], buf.at[slot], isem.at[slot]).start()

            @pl.when(i >= mine)
            def _():
                r = pl.multiple_of((i + shift) * TM, TM)
                pltpu.make_async_copy(sib_ref.at[:, pl.ds(r, TM), :], buf.at[slot], isem.at[slot]).start()

        def store(i, slot):
            for k in range(np_):
                here = i >= starts[k]
                if k + 1 < np_:
                    here = jnp.logical_and(here, i < starts[k + 1])

                @pl.when(here)
                def _():
                    r = pl.multiple_of((i - starts[k]) * TM, TM)
                    pltpu.make_async_copy(buf.at[slot], outs[k].at[:, pl.ds(r, TM), :], osem.at[slot]).start()

        def stored(slot):
            pltpu.make_async_copy(buf.at[slot], outs[0].at[:, pl.ds(0, TM), :], osem.at[slot]).wait()

        for s in range(3):

            @pl.when(s < n)
            def _():
                load(s, s)

        def body(i, _):
            slot = lax.rem(i, 4)
            pltpu.make_async_copy(own_ref.at[:, pl.ds(0, TM), :], buf.at[slot], isem.at[slot]).wait()
            store(i, slot)

            @pl.when(i >= 1)
            def _():
                stored(lax.rem(i + 3, 4))

            @pl.when(i + 3 < n)
            def _():
                load(i + 3, lax.rem(i + 3, 4))

            return 0

        lax.fori_loop(0, n, body, 0)

        @pl.when(n > 0)
        def _():
            stored(lax.rem(n + 3, 4))

    return pl.pallas_call(
        kern,
        in_specs=[SM, ANY, ANY],
        out_specs=[ANY] * np_,
        out_shape=[jax.ShapeDtypeStruct((2, k * TM, D), BF) for k in (FIRST, *PIECES)],
        scratch_shapes=[pltpu.VMEM((4, 2, TM, D), BF), pltpu.SemaphoreType.DMA((4,)), pltpu.SemaphoreType.DMA((4,))],
        compiler_params=pltpu.CompilerParams(vmem_limit_bytes=GRANT),
        cost_estimate=cost(10_000_000_000, 36_000_000),
        name="build_send",
    )(info, own, sib)


def gelu_and_slope(u):
    u2 = u * u
    t = jnp.tanh(u * (C1 + (C1 * C3) * u2))
    half = 0.5 + 0.5 * t
    act = u * half
    slope = half + (0.5 * u) * (1.0 - t * t) * (C1 + (3 * C1 * C3) * u2)
    return act, slope


def pick(e, lo, hi, fn):
    if hi - lo == 1:
        fn(lo)
        return
    mid = (lo + hi) // 2

    @pl.when(e < mid * 32)
    def _():
        pick(e, lo, mid, fn)

    @pl.when(e >= mid * 32)
    def _():
        pick(e, mid, hi, fn)


def issue_group(tab_ref, g, slot, src, xb, db, sem):
    for s in range(G):
        e = tab_ref[g * G + s]
        r = pl.multiple_of(lax.rem(e, 32) * TM, TM)

        def fetch(k):
            rows = pl.ds(s * TM, TM)
            pltpu.make_async_copy(src[k].at[0, pl.ds(r, TM), :], xb.at[slot, rows, :], sem.at[slot, 0]).start()
            pltpu.make_async_copy(src[k].at[1, pl.ds(r, TM), :], db.at[slot, rows, :], sem.at[slot, 1]).start()

        pick(e, 0, len(src), fetch)


def wait_group(slot, xb, db, sem):
    pltpu.make_async_copy(xb.at[slot], xb.at[slot], sem.at[slot, 0]).wait()
    pltpu.make_async_copy(db.at[slot], db.at[slot], sem.at[slot, 1]).wait()


def add_group(x, dy, wu, wd, gd, gu):
    u = lax.dot_general(wu[...], x, (((0,), (1,)), ((), ())), preferred_element_type=F32).astype(BF).astype(F32)
    da = lax.dot_general(wd[...], dy, (((1,), (1,)), ((), ())), preferred_element_type=F32)
    act, slope = gelu_and_slope(u)
    dh = (da * slope).astype(BF)
    gd[...] += jnp.dot(act.astype(BF), dy, preferred_element_type=F32)
    gu[...] += jnp.dot(dh, x, preferred_element_type=F32)


def weight_copies(c, lo, f, w, wub, wdb, sem):
    own, sib, fx, fd, wd_own, wd_oth = w
    cps = []
    c0, co = c * HB, (c - lo) * HB
    if not isinstance(c, int):
        c0, co = pl.multiple_of(c0, HB), pl.multiple_of(co, HB)
    for a in range(2):
        for k, (ref, col) in enumerate(((own, c0), (sib, c0), (fx, co), (fd, co))):
            rows = pl.ds(pl.multiple_of((f ^ k) * 512, 512), 512)
            cps.append(
                pltpu.make_async_copy(ref.at[a, :, pl.ds(col, HB)], wub.at[rows, pl.ds(a * HB, HB)], sem.at[k, a])
            )
    cps.append(pltpu.make_async_copy(wd_own.at[pl.ds(c0, HB), :], wdb.at[pl.ds(0, HB), :], sem.at[4, 0]))
    cps.append(pltpu.make_async_copy(wd_oth.at[pl.ds(co, HB), :], wdb.at[pl.ds(HB, HB), :], sem.at[4, 1]))
    return cps


def gather_scratch(n_acc):
    return [
        pltpu.VMEM((2, M, D), BF),
        pltpu.VMEM((2, M, D), BF),
        pltpu.VMEM((n_acc, D, FB), BF),
        pltpu.VMEM((n_acc, FB, D), BF),
        pltpu.VMEM((n_acc, FB, D), F32),
        pltpu.VMEM((n_acc, FB, D), F32),
        pltpu.SemaphoreType.DMA((2, 2)),
        pltpu.SemaphoreType.DMA((n_acc, 5, 2)),
    ]


def early_grads(tab, info, srcs, w, w_lo, lo_chunk, n_chunks, deps=()):
    ns = len(srcs)

    def kern(tab_ref, info_ref, *refs):
        src, wrefs, refs = refs[:ns], refs[ns : ns + 6], refs[ns + 6 + len(deps) :]
        out_d, out_u, xb, db, wub, wdb, gd, gu, sem, wsem, asem = refs
        groups, f = info_ref[0], info_ref[1]

        def weights(q, slot):
            return weight_copies(lo_chunk + q, w_lo, f, wrefs, wub.at[slot], wdb.at[slot], wsem.at[slot])

        def results(q, slot):
            return (
                pltpu.make_async_copy(gd.at[slot], out_d.at[q], asem.at[slot, 0]),
                pltpu.make_async_copy(gu.at[slot], out_u.at[q], asem.at[slot, 1]),
            )

        issue_group(tab_ref, 0, 0, src, xb, db, sem)
        for cp in weights(0, 0):
            cp.start()

        def chunk(q, t):
            ws = lax.rem(q, 2)

            @pl.when(q + 1 < n_chunks)
            def _():
                for cp in weights(q + 1, 1 - ws):
                    cp.start()

            @pl.when(q >= 2)
            def _():
                for cp in results(q - 2, ws):
                    cp.wait()

            gd[ws] = jnp.zeros((FB, D), F32)
            gu[ws] = jnp.zeros((FB, D), F32)
            for cp in weights(q, ws):
                cp.wait()

            def group(g, t):
                slot = lax.rem(t, 2)
                last = g + 1 == groups

                @pl.when(jnp.logical_or(jnp.logical_not(last), q + 1 < n_chunks))
                def _():
                    issue_group(tab_ref, jnp.where(last, 0, g + 1), 1 - slot, src, xb, db, sem)

                wait_group(slot, xb, db, sem)
                add_group(xb[slot], db[slot], wub.at[ws], wdb.at[ws], gd.at[ws], gu.at[ws])
                return t + 1

            t = lax.fori_loop(0, groups, group, t)
            for cp in results(q, ws):
                cp.start()
            return t

        lax.fori_loop(0, n_chunks, chunk, 0)
        for q in range(max(n_chunks - 2, 0), n_chunks):
            for cp in results(q, q % 2):
                cp.wait()

    return pl.pallas_call(
        kern,
        in_specs=[SM, SM] + [ANY] * (ns + 6) + [SM] * len(deps),
        out_specs=[ANY] * 2,
        out_shape=[jax.ShapeDtypeStruct((n_chunks, FB, D), F32)] * 2,
        scratch_shapes=gather_scratch(2) + [pltpu.SemaphoreType.DMA((2, 2))],
        compiler_params=pltpu.CompilerParams(vmem_limit_bytes=GRANT),
        cost_estimate=cost(8 * 5632 * D * FB * n_chunks, 60_000_000 * n_chunks),
    )(tab, info, *srcs, *w, *deps)


def chunk_grads(j, w_lo, tab, info, skip, srcs, w, prior, at, deps):
    ns = len(srcs)

    def kern(tab_ref, info_ref, *refs):
        src, refs = refs[:ns], refs[ns:]
        wrefs, (pd, pu), refs = refs[:6], refs[6:8], refs[8 + len(deps) :]
        keep_d, send_d, keep_u, send_u, xb, db, wub, wdb, gd, gu, sem, wsem, osem = refs
        groups, xi, f = info_ref[0], info_ref[1], info_ref[2]
        wub, wdb, gd, gu = wub.at[0], wdb.at[0], gd.at[0], gu.at[0]

        @pl.when(groups > skip)
        def _():
            issue_group(tab_ref, skip, 0, src, xb, db, sem)

        cps = weight_copies(j, w_lo, f, wrefs, wub, wdb, wsem.at[0])
        cps.append(pltpu.make_async_copy(pd.at[at], gd, osem.at[0]))
        cps.append(pltpu.make_async_copy(pu.at[at], gu, osem.at[1]))
        for cp in cps:
            cp.start()
        for cp in cps:
            cp.wait()

        def body(g, _):
            slot = lax.rem(g - skip, 2)

            @pl.when(g + 1 < groups)
            def _():
                issue_group(tab_ref, g + 1, 1 - slot, src, xb, db, sem)

            wait_group(slot, xb, db, sem)
            add_group(xb[slot], db[slot], wub, wdb, gd, gu)
            return 0

        lax.fori_loop(skip, groups, body, 0)
        kc = pl.multiple_of(xi * HALF, HALF)
        sc = pl.multiple_of((1 - xi) * HALF, HALF)
        ocp = [(gd.at[pl.ds(HB, HB), :], send_d), (gd.at[pl.ds(0, HB), :], keep_d)]
        for a in range(2):
            rows, cols = pl.ds(a * HB, HB), pl.ds(a * HALF, HALF)
            ocp.append((gu.at[rows, pl.ds(sc, HALF)], send_u.at[:, cols]))
            ocp.append((gu.at[rows, pl.ds(kc, HALF)], keep_u.at[:, cols]))
        ocp = [pltpu.make_async_copy(a, b, osem.at[i]) for i, (a, b) in enumerate(ocp)]
        for cp in ocp:
            cp.start()
        for cp in ocp:
            cp.wait()

    return pl.pallas_call(
        kern,
        in_specs=[SM, SM] + [ANY] * (ns + 8 + len(deps)),
        out_specs=[ANY] * 4,
        out_shape=[jax.ShapeDtypeStruct((HB, D), F32)] * 4,
        scratch_shapes=gather_scratch(1) + [pltpu.SemaphoreType.DMA((6,))],
        compiler_params=pltpu.CompilerParams(vmem_limit_bytes=GRANT),
        cost_estimate=cost(8 * 3072 * D * FB, 40_000_000),
    )(tab, info, *srcs, *w, *prior, *deps)


def finish_down(j, pos, keep, recv, out):
    first = out is None

    def kern(pos_ref, kd, rc, *refs):
        out_d, fd, vd, sem = refs if first else refs[1:]
        y = pos_ref[0]
        vd[...] = kd[...] + rc[...]
        row = pl.multiple_of(y * HALF + j * HB, HB)
        cps = [
            pltpu.make_async_copy(vd, fd, sem.at[0]),
            pltpu.make_async_copy(vd, out_d.at[pl.ds(row, HB), :], sem.at[1]),
        ]
        for cp in cps:
            cp.start()
        for cp in cps:
            cp.wait()

    extra = [] if first else [out]
    return pl.pallas_call(
        kern,
        in_specs=[SM, VM, VM] + [ANY] * len(extra),
        out_specs=[ANY] * 2,
        out_shape=[jax.ShapeDtypeStruct((D, D), F32), jax.ShapeDtypeStruct((HB, D), F32)],
        scratch_shapes=[pltpu.VMEM((HB, D), F32), pltpu.SemaphoreType.DMA((2,))],
        input_output_aliases={} if first else {3: 0},
        compiler_params=pltpu.CompilerParams(vmem_limit_bytes=16 * MIB),
        cost_estimate=cost(2_000_000_000, 4_000_000),
    )(pos, keep, recv, *extra)


def finish_up(j, pos, keep, recv, out):
    first = out is None

    def kern(pos_ref, ku, rc, *refs):
        out_u, fuc, fus, vu, sem = refs if first else refs[1:]
        y, xi, c = pos_ref[0], pos_ref[1], pos_ref[2]
        mine = pl.ds(pl.multiple_of(c * 512, 512), 512)
        other = pl.ds(pl.multiple_of((1 - c) * 512, 512), 512)
        vu[0] = (ku[:, 0:HALF] + rc[:, HALF:D]).T
        vu[1] = (ku[:, HALF:D] + rc[:, 0:HALF]).T
        cps = [
            pltpu.make_async_copy(vu.at[:, other, :], fus, sem.at[0]),
            pltpu.make_async_copy(vu.at[:, mine, :], fuc, sem.at[1]),
        ]
        for a in range(2):
            xa = xi if a == 0 else 1 - xi
            col = pl.multiple_of(((2 * xa + c) * 2 + y) * HALF + j * HB, HB)
            cps.append(pltpu.make_async_copy(vu.at[a, mine, :], out_u.at[:, pl.ds(col, HB)], sem.at[2 + a]))
        for cp in cps:
            cp.start()
        for cp in cps:
            cp.wait()

    extra = [] if first else [out]
    return pl.pallas_call(
        kern,
        in_specs=[SM, VM, VM] + [ANY] * len(extra),
        out_specs=[ANY] * 3,
        out_shape=[
            jax.ShapeDtypeStruct((512, 4 * D), F32),
            jax.ShapeDtypeStruct((2, 512, HB), F32),
            jax.ShapeDtypeStruct((2, 512, HB), F32),
        ],
        scratch_shapes=[pltpu.VMEM((2, HALF, HB), F32), pltpu.SemaphoreType.DMA((4,))],
        input_output_aliases={} if first else {3: 0},
        compiler_params=pltpu.CompilerParams(vmem_limit_bytes=16 * MIB),
        cost_estimate=cost(2_000_000_000, 4_000_000),
    )(pos, keep, recv, *extra)


def store(j, pos, rd, ruc, ruy, rus, outs):
    def kern(pos_ref, d_ref, uc_ref, uy_ref, us_ref, _d, _u, out_d, out_u, vd, vu, isem, osem):
        y, xi, c = pos_ref[0], pos_ref[1], pos_ref[2]
        row = pl.multiple_of((1 - y) * HALF + j * HB, HB)
        work = [(d_ref, vd, [(vd, out_d.at[pl.ds(row, HB), :])])]
        for k, (ref, cc, yy) in enumerate(((uc_ref, c, 1 - y), (uy_ref, 1 - c, 1 - y), (us_ref, 1 - c, y))):
            puts = []
            for a in range(2):
                xa = xi if a == 0 else 1 - xi
                col = pl.multiple_of(((2 * xa + cc) * 2 + yy) * HALF + j * HB, HB)
                puts.append((vu.at[k, a], out_u.at[:, pl.ds(col, HB)]))
            work.append((ref, vu.at[k], puts))
        loads = [pltpu.make_async_copy(src, mid, isem.at[n]) for n, (src, mid, _) in enumerate(work)]
        for cp in loads:
            cp.start()
        done = []
        for cp, (_, _, puts) in zip(loads, work):
            cp.wait()
            for src, dst in puts:
                put = pltpu.make_async_copy(src, dst, osem.at[len(done)])
                put.start()
                done.append(put)
        for put in done:
            put.wait()

    return pl.pallas_call(
        kern,
        in_specs=[SM] + [ANY] * 6,
        out_specs=[ANY] * 2,
        out_shape=[jax.ShapeDtypeStruct((D, D), F32), jax.ShapeDtypeStruct((512, 4 * D), F32)],
        scratch_shapes=[
            pltpu.VMEM((HB, D), F32),
            pltpu.VMEM((3, 2, 512, HB), F32),
            pltpu.SemaphoreType.DMA((4,)),
            pltpu.SemaphoreType.DMA((7,)),
        ],
        input_output_aliases={5: 0, 6: 1},
        compiler_params=pltpu.CompilerParams(vmem_limit_bytes=16 * MIB),
        cost_estimate=cost(3_000_000_000, 5_000_000),
    )(pos, rd, ruc, ruy, rus, *outs)


def nothing(k):
    return pl.pallas_call(lambda o: None, out_specs=ANY, out_shape=jax.ShapeDtypeStruct((2, k * TM, D), BF))()


def present(n):
    return (n >= 4, n >= 8, n >= 12, n % 4 >= 2, n % 2 == 1)


def exchange_branch(n, early):
    def run(pieces, *rest):
        got = []
        for k, here in enumerate(present(n)):
            got.append(y_swap(pieces[k]) if here else nothing(PIECES[k]))
        acc = early(*rest)
        sib = []
        for k, here in enumerate(present(n)):
            sib.append(core_swap(got[k]) if here else nothing(PIECES[k]))
        return (*got, *sib, *acc)

    return run


def solution(mesh):
    tok_spec = P(None, ("model", "replica", "fsdp"), None)
    len_spec = P(None, ("model", "replica", "fsdp"))
    w_spec = P(None, ("model", "fsdp"), None)

    def group_grads(x_in, dy, lengths, w_up, w_down):
        y, f = lax.axis_index("replica"), lax.axis_index("fsdp")
        xi, c = f // 2, f % 2
        w_up, w_down = w_up[0], w_down[0]

        row = jnp.zeros((8, 128), jnp.int32).at[:MICRO, 0].set(lengths[:, 0].astype(jnp.int32))
        around, s1 = start(row, x_in, dy)
        s1 = s1.reshape(2, MICRO * BASE, D)
        s1_y = y_swap(s1)
        me = y * 4 + f
        lens = around[(me - jnp.arange(8)) % 8][:, :MICRO, 0]

        def cols(xd, cd, lo=0, n=HALF):
            own = lax.dynamic_slice(w_up, (0, ((2 * xd + cd) * 2 + y) * HALF + lo), (512, n))
            oth = lax.dynamic_slice(w_up, (0, ((2 * (1 - xd) + cd) * 2 + y) * HALF + lo), (512, n))
            return jnp.stack([own, oth])

        wd_own = lax.dynamic_slice(w_down, (y * HALF, 0), (HALF, D))
        from_s = core_swap(cols(xi, 1 - c))
        mine = cols(xi, c)
        wsets = []
        for lo, n in WSETS:
            a = x_swap(cols(1 - xi, c, lo * HB, n * HB))
            b = x_diag(cols(1 - xi, 1 - c, lo * HB, n * HB))
            d = x_swap(lax.dynamic_slice(w_down, (y * HALF + lo * HB, 0), (n * HB, D)))
            wsets.append((mine, from_s, a, b, wd_own, d))

        rest = lens - BASE
        r16 = (rest + 15) // 16 * 16
        tiles = (jnp.sum(r16, axis=1) + TM - 1) // TM
        my_rest = lax.dynamic_index_in_dim(rest, me, keepdims=False)
        my16 = lax.dynamic_index_in_dim(r16, me, keepdims=False)
        offs = jnp.concatenate([jnp.zeros((1,), jnp.int32), jnp.cumsum(my16)])
        both = tiles[0::2] + tiles[1::2]
        share = jnp.stack([(both + 1) // 2, both // 2], axis=1).reshape(8)
        which = jnp.sum(jnp.max(share) - FIRST > jnp.array(SIZES[:-1]))
        more = jnp.array(SIZES)[which]

        def at(v, i):
            return lax.dynamic_index_in_dim(v, i, keepdims=False)

        t_own, t_sib = at(tiles, me), at(tiles, me ^ 1)
        h_own = at(share, me)
        h_y, h_ys = at(share, me ^ 4), at(share, me ^ 5)
        at_f = [FIRST + 4 * jnp.minimum(more // 4, k) for k in range(4)]
        at_one = at_f[3] + more % 4 // 2 * 2
        starts = [at_f[0], at_f[1], at_f[2], at_f[3], at_one]

        packed = pack_rest(x_in, dy, my_rest, offs)
        packed_s = core_swap(packed)
        s1_s = core_swap(s1)
        pa, *pieces = build_send(packed, packed_s, jnp.stack([h_own, t_own, t_sib - h_own, *starts]).astype(jnp.int32))
        qa = y_swap(pa)

        i = jnp.arange(64)
        n_own = 12 + t_own + t_sib
        g_own = (n_own + G - 1) // G
        k = i - g_own * G
        tab = jnp.where(i < n_own, 3 * 32 + i - 12 - t_own, 2 * 32 + NT)
        tab = jnp.where(i < 12 + t_own, 2 * 32 + i - 12, tab)
        tab = jnp.where(i < 12, (i // 6) * 32 + i % 6, tab)
        tab = jnp.where((k >= 0) & (k < 12), (4 + k // 6) * 32 + k % 6, tab).astype(jnp.int32)
        info_own = jnp.stack([g_own, f]).astype(jnp.int32)
        info_all = jnp.stack([g_own + 3, f]).astype(jnp.int32)

        i = jnp.arange(56) - 12
        own_list = i < h_y
        t = jnp.where(own_list, i, i - h_y)
        late = 2 * 32 + t
        for n, lo in enumerate(starts):
            late = jnp.where(t >= lo, (3 + n) * 32 + t - lo, late)
        late = jnp.where(own_list, late, late + 6 * 32)
        late = jnp.where(i < h_y + h_ys, late, 14 * 32 + NT)
        late = jnp.where(i < 0, (i + 12) // 6 * 32 + (i + 12) % 6, late).astype(jnp.int32)
        info_late = jnp.stack([3 + (h_y + h_ys + G - 1) // G, xi, f]).astype(jnp.int32)
        pos = jnp.stack([y, xi, c]).astype(jnp.int32)

        own_srcs = (s1, s1_s, packed, packed_s)
        acc0 = early_grads(tab, info_own, own_srcs, wsets[0], 0, 0, 2)
        acc1 = early_grads(tab, info_own, own_srcs, wsets[1], 2, 2, 1, (late, info_late, pos))
        s1_ys = core_swap(s1_y)
        srcs = (*own_srcs, s1_y, s1_ys)
        acc2 = early_grads(tab, info_all, srcs, wsets[1], 2, 3, 1)

        def early(tab, info, srcs, w):
            return early_grads(tab, info, srcs, w, 4, 4, 4)

        got = lax.switch(
            which,
            [exchange_branch(n, early) for n in SIZES],
            pieces, tab, info_all, srcs, list(wsets[2]),
        )
        pieces, sib_pieces, acc3 = got[:5], got[5:10], got[10:]
        qas = core_swap(qa)
        srcs = (s1_y, s1_ys, qa, *pieces, qas, *sib_pieces, packed)
        prior = [(acc0, 0), (acc0, 1), (acc1, 0), (acc2, 0), *((acc3, k) for k in range(4))]

        out_d = out_u = None
        fin = []
        for p, j in enumerate(ORDER):
            deps = (fin[p - 2][0],) if p >= 2 else ()
            w_at = next(h for h, (lo, n) in enumerate(WSETS) if lo <= j < lo + n)
            keep_d, send_d, keep_u, send_u = chunk_grads(
                j, WSETS[w_at][0], late, info_late, 0 if j < OWN_ONLY else 3, srcs, wsets[w_at], *prior[j], deps
            )
            recv_d = x_swap(send_d)
            recv_u = x_swap(send_u)
            out_d, fd = finish_down(j, pos, keep_d, recv_d, out_d)
            rd = y_swap(fd)
            out_u, fuc, fus = finish_up(j, pos, keep_u, recv_u, out_u)
            ruc = y_swap(fuc)
            ruy = y_diag(fus)
            rus = core_swap(fus)
            fin.append((fd, (rd, ruc, ruy, rus)))
            if p >= LAG:
                out_d, out_u = store(ORDER[p - LAG], pos, *fin[p - LAG][1], (out_d, out_u))
        for p in range(NCH - LAG, NCH):
            out_d, out_u = store(ORDER[p], pos, *fin[p][1], (out_d, out_u))
        return out_u[None], out_d[None]


    return jax.shard_map(
        group_grads,
        mesh=mesh,
        in_specs=(tok_spec, tok_spec, len_spec, w_spec, w_spec),
        out_specs=(w_spec, w_spec),
        check_vma=False,
    )
```

```python
import jax
import jax.numpy as jnp
from jax import lax
from jax.experimental import pallas as pl
from jax.experimental.pallas import tpu as pltpu
from jax.sharding import PartitionSpec as P


D = 2048
TOK = 1024
MICRO = 3
BASE = 256
REST = TOK - BASE
TM = 128
NT = MICRO * REST // TM
RROWS = MICRO * REST + TM
FIRST = 3
PIECES = (4, 4, 3, 2, 1, 1)
SIZES = (5, 7, 8, 9, 10, 11, 12, 15)
PARTS = ((0, 4), (0, 3, 4), (0, 2, 4), (0, 1, 4), (0, 1, 4, 5), (0, 1, 3, 4), (0, 1, 2, 4), (0, 1, 2, 3, 4, 5))
G = 4
M = G * TM
FB = 256
HB = FB // 2
NCH = D // FB
HALF = 1024
WSETS = ((0, 2), (2, 2), (4, 4))
ORDER = (3, 4, 0, 5, 6, 1, 7, 2)
LAG = 3
C1 = 0.7978845608028654
C3 = 0.044715
BF = jnp.bfloat16
F32 = jnp.float32


ANY = pl.BlockSpec(memory_space=pltpu.HBM)
SM = pl.BlockSpec(memory_space=pltpu.SMEM)
VM = pl.BlockSpec(memory_space=pltpu.VMEM)
MIB = 1024 * 1024
GRANT = 60 * 1024 * 1024

CORE = [(0, 1), (1, 0), (2, 3), (3, 2)]
XSWAP = [(0, 2), (2, 0), (1, 3), (3, 1)]
XDIAG = [(0, 3), (3, 0), (1, 2), (2, 1)]
YSWAP = [(0, 1), (1, 0)]
YDIAG = [(r * 4 + f, (1 - r) * 4 + (f ^ 1)) for r in range(2) for f in range(4)]


def core_swap(v):
    return lax.ppermute(v, "fsdp", CORE)


def x_swap(v):
    return lax.ppermute(v, "fsdp", XSWAP)


def x_diag(v):
    return lax.ppermute(v, "fsdp", XDIAG)


def y_swap(v):
    return lax.ppermute(v, "replica", YSWAP)


def y_diag(v):
    return lax.ppermute(v, ("replica", "fsdp"), YDIAG)


def cost(flops, nbytes):
    return pl.CostEstimate(flops=flops, bytes_accessed=nbytes, transcendentals=0)


def start(lens, x_in, dy):
    def kern(len_ref, x_ref, d_ref, all_ref, s1_ref, land, buf, send, recv, isem, osem):
        r, f = lax.axis_index("replica"), lax.axis_index("fsdp")
        me = r * 4 + f
        loads = []
        for a, ref in enumerate((x_ref, d_ref)):
            cp = pltpu.make_async_copy(ref.at[:, pl.ds(0, BASE), :], buf.at[a], isem.at[a])
            cp.start()
            loads.append(cp)
        barrier = pltpu.get_barrier_semaphore()
        peers = []
        for k in range(1, 8):
            p = lax.rem(me + k, 8)
            peers.append((0, p // 4, lax.rem(p, 4)))
        for p in peers:
            pl.semaphore_signal(barrier, inc=1, device_id=p, device_id_type=pl.DeviceIdType.MESH)
        pl.semaphore_wait(barrier, 7)
        cps = []
        for k, p in enumerate(peers):
            cp = pltpu.make_async_remote_copy(
                src_ref=len_ref,
                dst_ref=land.at[k],
                send_sem=send.at[k],
                recv_sem=recv.at[k],
                device_id=p,
                device_id_type=pl.DeviceIdType.MESH,
            )
            cp.start()
            cps.append(cp)
        outs = []
        for a in range(2):
            loads[a].wait()
            cp = pltpu.make_async_copy(buf.at[a], s1_ref.at[a], osem.at[a])
            cp.start()
            outs.append(cp)
        for cp in cps:
            cp.wait()
        all_ref[0] = len_ref[...]
        for k in range(7):
            all_ref[k + 1] = land[k]
        for cp in outs:
            cp.wait()

    return pl.pallas_call(
        kern,
        in_specs=[VM, ANY, ANY],
        out_specs=[VM, ANY],
        out_shape=[jax.ShapeDtypeStruct((8, 8, 128), jnp.int32), jax.ShapeDtypeStruct((2, MICRO, BASE, D), BF)],
        scratch_shapes=[
            pltpu.VMEM((7, 8, 128), jnp.int32),
            pltpu.VMEM((2, MICRO, BASE, D), BF),
            pltpu.SemaphoreType.DMA((7,)),
            pltpu.SemaphoreType.DMA((7,)),
            pltpu.SemaphoreType.DMA((2,)),
            pltpu.SemaphoreType.DMA((2,)),
        ],
        compiler_params=pltpu.CompilerParams(collective_id=0, has_side_effects=True, vmem_limit_bytes=GRANT),
        cost_estimate=cost(10_000_000_000, 13_000_000),
        name="start",
    )(lens, x_in, dy)


def pack_rest(x_in, dy, rest, offs):
    def kern(rest_ref, offs_ref, x_ref, d_ref, out_ref, buf, zero, isem, osem, zsem):
        loads = []
        for k in range(MICRO):
            for a, ref in enumerate((x_ref, d_ref)):
                cp = pltpu.make_async_copy(ref.at[k, pl.ds(BASE, REST), :], buf.at[k, a], isem.at[k, a])
                cp.start()
                loads.append(cp)
        zero[...] = jnp.zeros_like(zero)
        for k in range(MICRO):
            for a in range(2):
                loads[2 * k + a].wait()
            n = rest_ref[k]
            ragged = pl.multiple_of(jnp.minimum(n // 16 * 16, REST - 16), 16)
            row = lax.broadcasted_iota(jnp.int32, (16, D), 0) + ragged
            blk = buf[k, 1, pl.ds(ragged, 16), :]
            buf[k, 1, pl.ds(ragged, 16), :] = jnp.where(row < n, blk, jnp.zeros_like(blk))
            o = pl.multiple_of(offs_ref[k], 16)
            cps = [
                pltpu.make_async_copy(buf.at[k, a], out_ref.at[a, pl.ds(o, REST), :], osem.at[a]) for a in range(2)
            ]
            for cp in cps:
                cp.start()
            for cp in cps:
                cp.wait()
        for o in (pl.multiple_of(offs_ref[MICRO], 16), MICRO * REST):
            cps = [pltpu.make_async_copy(zero, out_ref.at[a, pl.ds(o, TM), :], zsem.at[a]) for a in range(2)]
            for cp in cps:
                cp.start()
            for cp in cps:
                cp.wait()

    return pl.pallas_call(
        kern,
        in_specs=[SM, SM, ANY, ANY],
        out_specs=ANY,
        out_shape=jax.ShapeDtypeStruct((2, RROWS, D), BF),
        scratch_shapes=[
            pltpu.VMEM((MICRO, 2, REST, D), BF),
            pltpu.VMEM((TM, D), BF),
            pltpu.SemaphoreType.DMA((MICRO, 2)),
            pltpu.SemaphoreType.DMA((2,)),
            pltpu.SemaphoreType.DMA((2,)),
        ],
        compiler_params=pltpu.CompilerParams(vmem_limit_bytes=GRANT),
        cost_estimate=cost(15_000_000_000, 50_000_000),
        name="pack_rest",
    )(rest, offs, x_in, dy)


def build_send(own, sib, info):
    np_ = 1 + len(PIECES)

    def kern(info_ref, own_ref, sib_ref, *refs):
        outs, (buf, isem, osem) = refs[:np_], refs[np_:]
        n, mine, shift = info_ref[0], info_ref[1], info_ref[2]
        starts = [0] + [info_ref[3 + k] for k in range(len(PIECES))]

        def load(i, slot):
            @pl.when(i < mine)
            def _():
                r = pl.multiple_of(i * TM, TM)
                pltpu.make_async_copy(own_ref.at[:, pl.ds(r, TM), :], buf.at[slot], isem.at[slot]).start()

            @pl.when(i >= mine)
            def _():
                r = pl.multiple_of((i + shift) * TM, TM)
                pltpu.make_async_copy(sib_ref.at[:, pl.ds(r, TM), :], buf.at[slot], isem.at[slot]).start()

        def store(i, slot):
            for k in range(np_):
                here = i >= starts[k]
                if k + 1 < np_:
                    here = jnp.logical_and(here, i < starts[k + 1])

                @pl.when(here)
                def _():
                    r = pl.multiple_of((i - starts[k]) * TM, TM)
                    pltpu.make_async_copy(buf.at[slot], outs[k].at[:, pl.ds(r, TM), :], osem.at[slot]).start()

        def stored(slot):
            pltpu.make_async_copy(buf.at[slot], outs[0].at[:, pl.ds(0, TM), :], osem.at[slot]).wait()

        for s in range(3):

            @pl.when(s < n)
            def _():
                load(s, s)

        def body(i, _):
            slot = lax.rem(i, 4)
            pltpu.make_async_copy(own_ref.at[:, pl.ds(0, TM), :], buf.at[slot], isem.at[slot]).wait()
            store(i, slot)

            @pl.when(i >= 1)
            def _():
                stored(lax.rem(i + 3, 4))

            @pl.when(i + 3 < n)
            def _():
                load(i + 3, lax.rem(i + 3, 4))

            return 0

        lax.fori_loop(0, n, body, 0)

        @pl.when(n > 0)
        def _():
            stored(lax.rem(n + 3, 4))

    return pl.pallas_call(
        kern,
        in_specs=[SM, ANY, ANY],
        out_specs=[ANY] * np_,
        out_shape=[jax.ShapeDtypeStruct((2, k * TM, D), BF) for k in (FIRST, *PIECES)],
        scratch_shapes=[pltpu.VMEM((4, 2, TM, D), BF), pltpu.SemaphoreType.DMA((4,)), pltpu.SemaphoreType.DMA((4,))],
        compiler_params=pltpu.CompilerParams(vmem_limit_bytes=GRANT),
        cost_estimate=cost(10_000_000_000, 36_000_000),
        name="build_send",
    )(info, own, sib)


def gelu_and_slope(u):
    u2 = u * u
    t = jnp.tanh(u * (C1 + (C1 * C3) * u2))
    half = 0.5 + 0.5 * t
    act = u * half
    slope = half + (0.5 * u) * (1.0 - t * t) * (C1 + (3 * C1 * C3) * u2)
    return act, slope


def pick(e, lo, hi, fn):
    if hi - lo == 1:
        fn(lo)
        return
    mid = (lo + hi) // 2

    @pl.when(e < mid * 32)
    def _():
        pick(e, lo, mid, fn)

    @pl.when(e >= mid * 32)
    def _():
        pick(e, mid, hi, fn)


def issue_group(tab_ref, g, slot, src, xb, db, sem):
    for s in range(G):
        e = tab_ref[g * G + s]
        r = pl.multiple_of(lax.rem(e, 32) * TM, TM)

        def fetch(k):
            rows = pl.ds(s * TM, TM)
            pltpu.make_async_copy(src[k].at[0, pl.ds(r, TM), :], xb.at[slot, rows, :], sem.at[slot, 0]).start()
            pltpu.make_async_copy(src[k].at[1, pl.ds(r, TM), :], db.at[slot, rows, :], sem.at[slot, 1]).start()

        pick(e, 0, len(src), fetch)


def wait_group(slot, xb, db, sem):
    pltpu.make_async_copy(xb.at[slot], xb.at[slot], sem.at[slot, 0]).wait()
    pltpu.make_async_copy(db.at[slot], db.at[slot], sem.at[slot, 1]).wait()


def add_group(x, dy, wu, wd, gd, gu):
    u = lax.dot_general(wu[...], x, (((0,), (1,)), ((), ())), preferred_element_type=F32).astype(BF).astype(F32)
    da = lax.dot_general(wd[...], dy, (((1,), (1,)), ((), ())), preferred_element_type=F32)
    act, slope = gelu_and_slope(u)
    dh = (da * slope).astype(BF)
    gd[...] += jnp.dot(act.astype(BF), dy, preferred_element_type=F32)
    gu[...] += jnp.dot(dh, x, preferred_element_type=F32)


def weight_copies(c, lo, at, w, wub, wdb, sem):
    w_up, sib, fx, fd, w_down, wd_oth = w
    y, f = at
    xi, core = f // 2, f % 2
    cps = []
    c0, co = c * HB, (c - lo) * HB
    if not isinstance(c, int):
        c0, co = pl.multiple_of(c0, HB), pl.multiple_of(co, HB)
    for a in range(2):
        xa = xi if a == 0 else 1 - xi
        col = pl.multiple_of(((2 * xa + core) * 2 + y) * HALF + c0, HB)
        parts = [w_up.at[:, pl.ds(col, HB)], sib.at[a, :, pl.ds(c0, HB)]]
        parts += [ref.at[a, :, pl.ds(co, HB)] for ref in (fx, fd)]
        for k, part in enumerate(parts):
            rows = pl.ds(pl.multiple_of((f ^ k) * 512, 512), 512)
            cps.append(pltpu.make_async_copy(part, wub.at[rows, pl.ds(a * HB, HB)], sem.at[k, a]))
    own = pl.ds(pl.multiple_of(y * HALF + c0, HB), HB)
    cps.append(pltpu.make_async_copy(w_down.at[own, :], wdb.at[pl.ds(0, HB), :], sem.at[4, 0]))
    cps.append(pltpu.make_async_copy(wd_oth.at[pl.ds(co, HB), :], wdb.at[pl.ds(HB, HB), :], sem.at[4, 1]))
    return cps


def gather_scratch(n_acc):
    return [
        pltpu.VMEM((2, M, D), BF),
        pltpu.VMEM((2, M, D), BF),
        pltpu.VMEM((n_acc, D, FB), BF),
        pltpu.VMEM((n_acc, FB, D), BF),
        pltpu.VMEM((n_acc, FB, D), F32),
        pltpu.VMEM((n_acc, FB, D), F32),
        pltpu.SemaphoreType.DMA((2, 2)),
        pltpu.SemaphoreType.DMA((n_acc, 5, 2)),
    ]


def early_grads(tab, info, srcs, wsets, lo_chunk, n_new, prior=(), deps=()):
    ns, nw, npr = len(srcs), len(wsets), len(prior)
    sizes = [p[0].shape[0] for p in prior]
    n_chunks = n_new + sum(sizes)

    def kern(tab_ref, info_ref, *refs):
        src, refs = refs[:ns], refs[ns:]
        wrefs, refs = [refs[6 * k : 6 * k + 6] for k in range(nw)], refs[6 * nw :]
        pri, refs = refs[: 2 * npr], refs[2 * npr + len(deps) :]
        out_d, out_u, xb, db, wub, wdb, gd, gu, sem, wsem, asem = refs
        hi, at = info_ref[1], (info_ref[2], info_ref[3])

        def lo(q):
            return jnp.where(q < n_new, 0, info_ref[0])

        def weights(q, slot, act):
            c = jnp.where(q < n_new, lo_chunk + q, q - n_new) if npr else lo_chunk + q

            def act_all(k):
                for cp in weight_copies(c, wsets[k][0], at, wrefs[k], wub.at[slot], wdb.at[slot], wsem.at[slot]):
                    act(cp)

            if nw == 1:
                act_all(0)
                return
            for k in range(nw):
                first, count, _ = wsets[k]

                @pl.when(jnp.logical_and(c >= first, c < first + count))
                def _():
                    act_all(k)

        def start_copy(cp):
            cp.start()

        def wait_copy(cp):
            cp.wait()

        def results(q, slot):
            return (
                pltpu.make_async_copy(gd.at[slot], out_d.at[q], asem.at[slot, 0]),
                pltpu.make_async_copy(gu.at[slot], out_u.at[q], asem.at[slot, 1]),
            )

        issue_group(tab_ref, lo(0), 0, src, xb, db, sem)
        weights(0, 0, start_copy)

        def chunk(q, t):
            ws = lax.rem(q, 2)

            @pl.when(q + 1 < n_chunks)
            def _():
                weights(q + 1, 1 - ws, start_copy)

            @pl.when(q >= 2)
            def _():
                for cp in results(q - 2, ws):
                    cp.wait()

            @pl.when(q < n_new)
            def _():
                gd[ws] = jnp.zeros((FB, D), F32)
                gu[ws] = jnp.zeros((FB, D), F32)

            base = n_new
            for k in range(npr):
                first, base = base, base + sizes[k]

                @pl.when(jnp.logical_and(q >= first, q < base))
                def _():
                    cps = (
                        pltpu.make_async_copy(pri[2 * k].at[q - first], gd.at[ws], asem.at[ws, 0]),
                        pltpu.make_async_copy(pri[2 * k + 1].at[q - first], gu.at[ws], asem.at[ws, 1]),
                    )
                    for cp in cps:
                        cp.start()
                    for cp in cps:
                        cp.wait()

            weights(q, ws, wait_copy)

            def group(g, t):
                slot = lax.rem(t, 2)
                last = g + 1 == hi

                @pl.when(jnp.logical_or(jnp.logical_not(last), q + 1 < n_chunks))
                def _():
                    issue_group(tab_ref, jnp.where(last, lo(q + 1), g + 1), 1 - slot, src, xb, db, sem)

                wait_group(slot, xb, db, sem)
                add_group(xb[slot], db[slot], wub.at[ws], wdb.at[ws], gd.at[ws], gu.at[ws])
                return t + 1

            t = lax.fori_loop(lo(q), hi, group, t)
            for cp in results(q, ws):
                cp.start()
            return t

        lax.fori_loop(0, n_chunks, chunk, 0)
        for q in range(max(n_chunks - 2, 0), n_chunks):
            for cp in results(q, q % 2):
                cp.wait()

    flat = [a for _, _, w in wsets for a in w]
    pri = [a for p in prior for a in p]
    return pl.pallas_call(
        kern,
        in_specs=[SM, SM] + [ANY] * (ns + len(flat) + len(pri)) + [SM] * len(deps),
        out_specs=[ANY] * 2,
        out_shape=[jax.ShapeDtypeStruct((n_chunks, FB, D), F32)] * 2,
        scratch_shapes=gather_scratch(2) + [pltpu.SemaphoreType.DMA((2, 2))],
        compiler_params=pltpu.CompilerParams(vmem_limit_bytes=GRANT),
        cost_estimate=cost(8 * 5632 * D * FB * n_new, 60_000_000 * n_new),
    )(tab, info, *srcs, *flat, *pri, *deps)


def chunk_grads(j, tab, info, srcs, wset, prior, at, deps):
    ns = len(srcs)
    w_lo, _, w = wset

    def kern(tab_ref, info_ref, *refs):
        src, refs = refs[:ns], refs[ns:]
        wrefs, (pd, pu), refs = refs[:6], refs[6:8], refs[8 + len(deps) :]
        keep_d, send_d, keep_u, send_u, xb, db, wub, wdb, gd, gu, sem, wsem, osem = refs
        groups, y, f = info_ref[0], info_ref[1], info_ref[2]
        xi = f // 2
        wub, wdb, gd, gu = wub.at[0], wdb.at[0], gd.at[0], gu.at[0]

        @pl.when(groups > 0)
        def _():
            issue_group(tab_ref, 0, 0, src, xb, db, sem)

        cps = weight_copies(j, w_lo, (y, f), wrefs, wub, wdb, wsem.at[0])
        cps.append(pltpu.make_async_copy(pd.at[at], gd, osem.at[0]))
        cps.append(pltpu.make_async_copy(pu.at[at], gu, osem.at[1]))
        for cp in cps:
            cp.start()
        for cp in cps:
            cp.wait()

        def body(g, _):
            slot = lax.rem(g, 2)

            @pl.when(g + 1 < groups)
            def _():
                issue_group(tab_ref, g + 1, 1 - slot, src, xb, db, sem)

            wait_group(slot, xb, db, sem)
            add_group(xb[slot], db[slot], wub, wdb, gd, gu)
            return 0

        lax.fori_loop(0, groups, body, 0)
        kc = pl.multiple_of(xi * HALF, HALF)
        sc = pl.multiple_of((1 - xi) * HALF, HALF)
        ocp = [(gd.at[pl.ds(HB, HB), :], send_d), (gd.at[pl.ds(0, HB), :], keep_d)]
        for a in range(2):
            rows, cols = pl.ds(a * HB, HB), pl.ds(a * HALF, HALF)
            ocp.append((gu.at[rows, pl.ds(sc, HALF)], send_u.at[:, cols]))
            ocp.append((gu.at[rows, pl.ds(kc, HALF)], keep_u.at[:, cols]))
        ocp = [pltpu.make_async_copy(a, b, osem.at[i]) for i, (a, b) in enumerate(ocp)]
        for cp in ocp:
            cp.start()
        for cp in ocp:
            cp.wait()

    return pl.pallas_call(
        kern,
        in_specs=[SM, SM] + [ANY] * (ns + 8 + len(deps)),
        out_specs=[ANY] * 4,
        out_shape=[jax.ShapeDtypeStruct((HB, D), F32)] * 4,
        scratch_shapes=gather_scratch(1) + [pltpu.SemaphoreType.DMA((6,))],
        compiler_params=pltpu.CompilerParams(vmem_limit_bytes=GRANT),
        cost_estimate=cost(8 * 3072 * D * FB, 40_000_000),
    )(tab, info, *srcs, *w, *prior, *deps)


def finish_down(j, pos, keep, recv, out):
    first = out is None

    def kern(pos_ref, kd, rc, *refs):
        out_d, fd, vd, sem = refs if first else refs[1:]
        y = pos_ref[0]
        vd[...] = kd[...] + rc[...]
        row = pl.multiple_of(y * HALF + j * HB, HB)
        cps = [
            pltpu.make_async_copy(vd, fd, sem.at[0]),
            pltpu.make_async_copy(vd, out_d.at[pl.ds(row, HB), :], sem.at[1]),
        ]
        for cp in cps:
            cp.start()
        for cp in cps:
            cp.wait()

    extra = [] if first else [out]
    return pl.pallas_call(
        kern,
        in_specs=[SM, VM, VM] + [ANY] * len(extra),
        out_specs=[ANY] * 2,
        out_shape=[jax.ShapeDtypeStruct((D, D), F32), jax.ShapeDtypeStruct((HB, D), F32)],
        scratch_shapes=[pltpu.VMEM((HB, D), F32), pltpu.SemaphoreType.DMA((2,))],
        input_output_aliases={} if first else {3: 0},
        compiler_params=pltpu.CompilerParams(vmem_limit_bytes=GRANT),
        cost_estimate=cost(2_000_000_000, 4_000_000),
    )(pos, keep, recv, *extra)


def finish_up(j, pos, keep, recv, out):
    first = out is None

    def kern(pos_ref, ku, rc, *refs):
        out_u, fuc, fus, vu, sem = refs if first else refs[1:]
        y, xi, c = pos_ref[0], pos_ref[1], pos_ref[2]
        mine = pl.ds(pl.multiple_of(c * 512, 512), 512)
        other = pl.ds(pl.multiple_of((1 - c) * 512, 512), 512)
        vu[0] = (ku[:, 0:HALF] + rc[:, HALF:D]).T
        vu[1] = (ku[:, HALF:D] + rc[:, 0:HALF]).T
        cps = [
            pltpu.make_async_copy(vu.at[:, other, :], fus, sem.at[0]),
            pltpu.make_async_copy(vu.at[:, mine, :], fuc, sem.at[1]),
        ]
        for a in range(2):
            xa = xi if a == 0 else 1 - xi
            col = pl.multiple_of(((2 * xa + c) * 2 + y) * HALF + j * HB, HB)
            cps.append(pltpu.make_async_copy(vu.at[a, mine, :], out_u.at[:, pl.ds(col, HB)], sem.at[2 + a]))
        for cp in cps:
            cp.start()
        for cp in cps:
            cp.wait()

    extra = [] if first else [out]
    return pl.pallas_call(
        kern,
        in_specs=[SM, VM, VM] + [ANY] * len(extra),
        out_specs=[ANY] * 3,
        out_shape=[
            jax.ShapeDtypeStruct((512, 4 * D), F32),
            jax.ShapeDtypeStruct((2, 512, HB), F32),
            jax.ShapeDtypeStruct((2, 512, HB), F32),
        ],
        scratch_shapes=[pltpu.VMEM((2, HALF, HB), F32), pltpu.SemaphoreType.DMA((4,))],
        input_output_aliases={} if first else {3: 0},
        compiler_params=pltpu.CompilerParams(vmem_limit_bytes=GRANT),
        cost_estimate=cost(2_000_000_000, 4_000_000),
    )(pos, keep, recv, *extra)


def store(j, pos, rd, ruc, ruy, rus, outs):
    def kern(pos_ref, d_ref, uc_ref, uy_ref, us_ref, _d, _u, out_d, out_u, vd, vu, isem, osem):
        y, xi, c = pos_ref[0], pos_ref[1], pos_ref[2]
        row = pl.multiple_of((1 - y) * HALF + j * HB, HB)
        work = [(d_ref, vd, [(vd, out_d.at[pl.ds(row, HB), :])])]
        for k, (ref, cc, yy) in enumerate(((uc_ref, c, 1 - y), (uy_ref, 1 - c, 1 - y), (us_ref, 1 - c, y))):
            puts = []
            for a in range(2):
                xa = xi if a == 0 else 1 - xi
                col = pl.multiple_of(((2 * xa + cc) * 2 + yy) * HALF + j * HB, HB)
                puts.append((vu.at[k, a], out_u.at[:, pl.ds(col, HB)]))
            work.append((ref, vu.at[k], puts))
        loads = [pltpu.make_async_copy(src, mid, isem.at[n]) for n, (src, mid, _) in enumerate(work)]
        for cp in loads:
            cp.start()
        done = []
        for cp, (_, _, puts) in zip(loads, work):
            cp.wait()
            for src, dst in puts:
                put = pltpu.make_async_copy(src, dst, osem.at[len(done)])
                put.start()
                done.append(put)
        for put in done:
            put.wait()

    return pl.pallas_call(
        kern,
        in_specs=[SM] + [ANY] * 6,
        out_specs=[ANY] * 2,
        out_shape=[jax.ShapeDtypeStruct((D, D), F32), jax.ShapeDtypeStruct((512, 4 * D), F32)],
        scratch_shapes=[
            pltpu.VMEM((HB, D), F32),
            pltpu.VMEM((3, 2, 512, HB), F32),
            pltpu.SemaphoreType.DMA((4,)),
            pltpu.SemaphoreType.DMA((7,)),
        ],
        input_output_aliases={5: 0, 6: 1},
        compiler_params=pltpu.CompilerParams(vmem_limit_bytes=16 * MIB),
        cost_estimate=cost(3_000_000_000, 5_000_000),
    )(pos, rd, ruc, ruy, rus, *outs)


def nothing(k):
    return pl.pallas_call(lambda o: None, out_specs=ANY, out_shape=jax.ShapeDtypeStruct((2, k * TM, D), BF))()


def exchange_branch(parts, early):
    here = [k in parts for k in range(len(PIECES))]

    def run(pieces, *rest):
        got = []
        for k in range(len(PIECES)):
            got.append(y_swap(pieces[k]) if here[k] else nothing(PIECES[k]))
        acc = early(*rest)
        sib = []
        for k in range(len(PIECES)):
            sib.append(core_swap(got[k]) if here[k] else nothing(PIECES[k]))
        return (*got, *sib, *acc)

    return run


def piece_starts():
    table = []
    for size, parts in zip(SIZES, PARTS):
        at, row = FIRST, []
        for k in range(len(PIECES)):
            row.append(at)
            at += PIECES[k] if k in parts else 0
        assert at == FIRST + size
        table.append(row)
    return table


def solution(mesh):
    tok_spec = P(None, ("model", "replica", "fsdp"), None)
    len_spec = P(None, ("model", "replica", "fsdp"))
    w_spec = P(None, ("model", "fsdp"), None)

    def group_grads(x_in, dy, lengths, w_up, w_down):
        y, f = lax.axis_index("replica"), lax.axis_index("fsdp")
        xi, c = f // 2, f % 2
        w_up, w_down = w_up[0], w_down[0]

        row = jnp.zeros((8, 128), jnp.int32).at[:MICRO, 0].set(lengths[:, 0].astype(jnp.int32))
        around, s1 = start(row, x_in, dy)
        s1 = s1.reshape(2, MICRO * BASE, D)
        s1_y = y_swap(s1)
        me = y * 4 + f
        lens = around[(me - jnp.arange(8)) % 8][:, :MICRO, 0]

        def cols(xd, cd, lo=0, n=HALF):
            own = lax.dynamic_slice(w_up, (0, ((2 * xd + cd) * 2 + y) * HALF + lo), (512, n))
            oth = lax.dynamic_slice(w_up, (0, ((2 * (1 - xd) + cd) * 2 + y) * HALF + lo), (512, n))
            return jnp.stack([own, oth])

        from_s = core_swap(cols(xi, 1 - c))
        wsets = []
        for lo, n in WSETS:
            a = x_swap(cols(1 - xi, c, lo * HB, n * HB))
            b = x_diag(cols(1 - xi, 1 - c, lo * HB, n * HB))
            d = x_swap(lax.dynamic_slice(w_down, (y * HALF + lo * HB, 0), (n * HB, D)))
            wsets.append((lo, n, [w_up, from_s, a, b, w_down, d]))

        rest = lens - BASE
        r16 = (rest + 15) // 16 * 16
        tiles = (jnp.sum(r16, axis=1) + TM - 1) // TM
        my_rest = lax.dynamic_index_in_dim(rest, me, keepdims=False)
        my16 = lax.dynamic_index_in_dim(r16, me, keepdims=False)
        offs = jnp.concatenate([jnp.zeros((1,), jnp.int32), jnp.cumsum(my16)])
        both = tiles[0::2] + tiles[1::2]
        share = jnp.stack([(both + 1) // 2, both // 2], axis=1).reshape(8)
        which = jnp.sum(jnp.max(share) - FIRST > jnp.array(SIZES[:-1]))
        starts = jnp.array(piece_starts())[which]

        def at(v, i):
            return lax.dynamic_index_in_dim(v, i, keepdims=False)

        t_own, t_sib = at(tiles, me), at(tiles, me ^ 1)
        h_own = at(share, me)
        h_y, h_ys = at(share, me ^ 4), at(share, me ^ 5)
        packed = pack_rest(x_in, dy, my_rest, offs)
        packed_s = core_swap(packed)
        s1_s = core_swap(s1)
        pa, *pieces = build_send(
            packed, packed_s, jnp.concatenate([jnp.stack([h_own, t_own, t_sib - h_own]), starts]).astype(jnp.int32)
        )
        qa = y_swap(pa)

        i = jnp.arange(64)
        n_own = 12 + t_own + t_sib
        g_own = (n_own + G - 1) // G
        k = i - g_own * G
        tab = jnp.where(i < n_own, 3 * 32 + i - 12 - t_own, 2 * 32 + NT)
        tab = jnp.where(i < 12 + t_own, 2 * 32 + i - 12, tab)
        tab = jnp.where(i < 12, (i // 6) * 32 + i % 6, tab)
        tab = jnp.where((k >= 0) & (k < 12), (4 + k // 6) * 32 + k % 6, tab).astype(jnp.int32)
        info_own = jnp.stack([0, g_own, y, f]).astype(jnp.int32)
        info_all = jnp.stack([g_own, g_own + 3, y, f]).astype(jnp.int32)

        i = jnp.arange(40)
        own_list = i < h_y
        t = jnp.where(own_list, i, i - h_y)
        late = t
        for n in range(len(PIECES)):
            late = jnp.where(t >= starts[n], (1 + n) * 32 + t - starts[n], late)
        late = jnp.where(own_list, late, late + (1 + len(PIECES)) * 32)
        late = jnp.where(i < h_y + h_ys, late, 2 * (1 + len(PIECES)) * 32 + NT).astype(jnp.int32)
        info_late = jnp.stack([(h_y + h_ys + G - 1) // G, y, f]).astype(jnp.int32)
        pos = jnp.stack([y, xi, c]).astype(jnp.int32)

        own_srcs = (s1, s1_s, packed, packed_s)
        acc0 = early_grads(tab, info_own, own_srcs, wsets[:1], 0, 2)
        acc1 = early_grads(tab, info_own, own_srcs, wsets[1:2], 2, 1, (), (late, info_late, pos))
        s1_ys = core_swap(s1_y)
        srcs = (*own_srcs, s1_y, s1_ys)
        acc2 = early_grads(tab, info_all, srcs, wsets[1:2], 3, 1)

        def early(tab, info, srcs, w, prior):
            sets = [(lo, n, v) for (lo, n), v in zip(WSETS, w)]
            return early_grads(tab, info, srcs, sets, 4, 4, prior)

        got = lax.switch(
            which,
            [exchange_branch(parts, early) for parts in PARTS],
            pieces, tab, info_all, srcs, [w for _, _, w in wsets], [list(acc0), list(acc1)],
        )
        k = len(PIECES)
        pieces, sib_pieces, acc3 = got[:k], got[k : 2 * k], got[2 * k :]
        qas = core_swap(qa)
        srcs = (qa, *pieces, qas, *sib_pieces, packed)
        prior = [(acc3, 4), (acc3, 5), (acc3, 6), (acc2, 0), *((acc3, k) for k in range(4))]

        out_d = out_u = None
        fin = []
        for p, j in enumerate(ORDER):
            deps = (fin[p - 2][0],) if p >= 2 else ()
            w_at = next(h for h, (lo, n) in enumerate(WSETS) if lo <= j < lo + n)
            keep_d, send_d, keep_u, send_u = chunk_grads(
                j, late, info_late, srcs, wsets[w_at], *prior[j], deps
            )
            recv_d = x_swap(send_d)
            recv_u = x_swap(send_u)
            out_d, fd = finish_down(j, pos, keep_d, recv_d, out_d)
            rd = y_swap(fd)
            out_u, fuc, fus = finish_up(j, pos, keep_u, recv_u, out_u)
            ruc = y_swap(fuc)
            ruy = y_diag(fus)
            rus = core_swap(fus)
            fin.append((fd, (rd, ruc, ruy, rus)))
            if p >= LAG:
                out_d, out_u = store(ORDER[p - LAG], pos, *fin[p - LAG][1], (out_d, out_u))
        for p in range(NCH - LAG, NCH):
            out_d, out_u = store(ORDER[p], pos, *fin[p][1], (out_d, out_u))
        return out_u[None], out_d[None]


    return jax.shard_map(
        group_grads,
        mesh=mesh,
        in_specs=(tok_spec, tok_spec, len_spec, w_spec, w_spec),
        out_specs=(w_spec, w_spec),
        check_vma=False,
    )
```

```python
import jax
import jax.numpy as jnp
from jax import lax
from jax.experimental import pallas as pl
from jax.experimental.pallas import tpu as pltpu
from jax.sharding import PartitionSpec as P


D = 2048
TOK = 1024
MICRO = 3
BASE = 256
REST = TOK - BASE
TM = 128
NT = MICRO * REST // TM
RROWS = MICRO * REST + TM
FIRST = 3
MAIN = (4, 4, 3, 2)
TAIL = 2
SIZES = (6, 7, 8, 9, 10, 11, 12, 15)
PARTS = ((0,), (2, 3), (0, 3), (0, 2), (0, 1), (0, 2, 3), (0, 1, 3), (0, 1, 2, 3))
G = 4
M = G * TM
FB = 256
HB = FB // 2
NCH = D // FB
HALF = 1024
WSETS = ((0, 2), (2, 2), (4, 4))
ORDER = (3, 4, 0, 5, 6, 1, 7, 2)
LAG = 3
C1 = 0.7978845608028654
C3 = 0.044715
BF = jnp.bfloat16
F32 = jnp.float32


ANY = pl.BlockSpec(memory_space=pltpu.HBM)
SM = pl.BlockSpec(memory_space=pltpu.SMEM)
VM = pl.BlockSpec(memory_space=pltpu.VMEM)
MIB = 1024 * 1024
GRANT = 60 * 1024 * 1024

CORE = [(0, 1), (1, 0), (2, 3), (3, 2)]
XSWAP = [(0, 2), (2, 0), (1, 3), (3, 1)]
XDIAG = [(0, 3), (3, 0), (1, 2), (2, 1)]
YSWAP = [(0, 1), (1, 0)]
YDIAG = [(r * 4 + f, (1 - r) * 4 + (f ^ 1)) for r in range(2) for f in range(4)]


def core_swap(v):
    return lax.ppermute(v, "fsdp", CORE)


def x_swap(v):
    return lax.ppermute(v, "fsdp", XSWAP)


def x_diag(v):
    return lax.ppermute(v, "fsdp", XDIAG)


def y_swap(v):
    return lax.ppermute(v, "replica", YSWAP)


def y_diag(v):
    return lax.ppermute(v, ("replica", "fsdp"), YDIAG)


def cost(flops, nbytes):
    return pl.CostEstimate(flops=flops, bytes_accessed=nbytes, transcendentals=0)


def start(lens, x_in, dy):
    def kern(len_ref, x_ref, d_ref, all_ref, s1_ref, land, buf, send, recv, isem, osem):
        r, f = lax.axis_index("replica"), lax.axis_index("fsdp")
        me = r * 4 + f
        loads = []
        for a, ref in enumerate((x_ref, d_ref)):
            cp = pltpu.make_async_copy(ref.at[:, pl.ds(0, BASE), :], buf.at[a], isem.at[a])
            cp.start()
            loads.append(cp)
        barrier = pltpu.get_barrier_semaphore()
        peers = []
        for k in range(1, 8):
            p = lax.rem(me + k, 8)
            peers.append((0, p // 4, lax.rem(p, 4)))
        for p in peers:
            pl.semaphore_signal(barrier, inc=1, device_id=p, device_id_type=pl.DeviceIdType.MESH)
        pl.semaphore_wait(barrier, 7)
        cps = []
        for k, p in enumerate(peers):
            cp = pltpu.make_async_remote_copy(
                src_ref=len_ref,
                dst_ref=land.at[k],
                send_sem=send.at[k],
                recv_sem=recv.at[k],
                device_id=p,
                device_id_type=pl.DeviceIdType.MESH,
            )
            cp.start()
            cps.append(cp)
        outs = []
        for a in range(2):
            loads[a].wait()
            cp = pltpu.make_async_copy(buf.at[a], s1_ref.at[a], osem.at[a])
            cp.start()
            outs.append(cp)
        for cp in cps:
            cp.wait()
        all_ref[0] = len_ref[...]
        for k in range(7):
            all_ref[k + 1] = land[k]
        for cp in outs:
            cp.wait()

    return pl.pallas_call(
        kern,
        in_specs=[VM, ANY, ANY],
        out_specs=[VM, ANY],
        out_shape=[jax.ShapeDtypeStruct((8, 8, 128), jnp.int32), jax.ShapeDtypeStruct((2, MICRO, BASE, D), BF)],
        scratch_shapes=[
            pltpu.VMEM((7, 8, 128), jnp.int32),
            pltpu.VMEM((2, MICRO, BASE, D), BF),
            pltpu.SemaphoreType.DMA((7,)),
            pltpu.SemaphoreType.DMA((7,)),
            pltpu.SemaphoreType.DMA((2,)),
            pltpu.SemaphoreType.DMA((2,)),
        ],
        compiler_params=pltpu.CompilerParams(collective_id=0, has_side_effects=True, vmem_limit_bytes=GRANT),
        cost_estimate=cost(10_000_000_000, 13_000_000),
        name="start",
    )(lens, x_in, dy)


def pack_rest(x_in, dy, rest, offs):
    per = REST // TM

    def kern(rest_ref, offs_ref, x_ref, d_ref, out_ref, buf, zero, isem, osem, zsem):
        def load(k, t):
            rows = pl.ds(BASE + t * TM, TM)
            return [
                pltpu.make_async_copy(ref.at[k, rows, :], buf.at[k, t, a], isem.at[k, t, a])
                for a, ref in enumerate((x_ref, d_ref))
            ]

        def put(k, t):
            o = pl.multiple_of(offs_ref[k] + t * TM, 16)
            return [
                pltpu.make_async_copy(buf.at[k, t, a], out_ref.at[a, pl.ds(o, TM), :], osem.at[t, a]) for a in range(2)
            ]

        def each(k, fn):
            for t in range(per):

                @pl.when(t * TM < rest_ref[k])
                def _():
                    fn(k, t)

        def begin(k, t):
            for cp in load(k, t):
                cp.start()

        def move(k, t):
            for cp in load(k, t):
                cp.wait()
            n = rest_ref[k] - t * TM

            @pl.when(n < TM)
            def _():
                ragged = pl.multiple_of(n // 16 * 16, 16)
                row = lax.broadcasted_iota(jnp.int32, (16, D), 0) + ragged
                blk = buf[k, t, 1, pl.ds(ragged, 16), :]
                buf[k, t, 1, pl.ds(ragged, 16), :] = jnp.where(row < n, blk, jnp.zeros_like(blk))

            for cp in put(k, t):
                cp.start()

        def end(k, t):
            for cp in put(k, t):
                cp.wait()

        for k in range(MICRO):
            each(k, begin)
        zero[...] = jnp.zeros_like(zero)
        for k in range(MICRO):
            each(k, move)
            each(k, end)
        for o in (pl.multiple_of(offs_ref[MICRO], 16), MICRO * REST):
            cps = [pltpu.make_async_copy(zero, out_ref.at[a, pl.ds(o, TM), :], zsem.at[a]) for a in range(2)]
            for cp in cps:
                cp.start()
            for cp in cps:
                cp.wait()

    return pl.pallas_call(
        kern,
        in_specs=[SM, SM, ANY, ANY],
        out_specs=ANY,
        out_shape=jax.ShapeDtypeStruct((2, RROWS, D), BF),
        scratch_shapes=[
            pltpu.VMEM((MICRO, per, 2, TM, D), BF),
            pltpu.VMEM((TM, D), BF),
            pltpu.SemaphoreType.DMA((MICRO, per, 2)),
            pltpu.SemaphoreType.DMA((per, 2)),
            pltpu.SemaphoreType.DMA((2,)),
        ],
        compiler_params=pltpu.CompilerParams(vmem_limit_bytes=GRANT),
        cost_estimate=cost(15_000_000_000, 50_000_000),
        name="pack_rest",
    )(rest, offs, x_in, dy)


def build_send(own, sib, info):
    sizes = (FIRST, *MAIN, TAIL, TAIL)
    np_ = len(sizes)

    def kern(info_ref, own_ref, sib_ref, *refs):
        outs, (buf, isem, osem) = refs[:np_], refs[np_:]
        n, keep, mine, shift = info_ref[0], info_ref[1], info_ref[2], info_ref[3]
        starts = [0] + [info_ref[4 + k] for k in range(np_ - 2)]

        def load(i, slot):
            @pl.when(i < mine)
            def _():
                r = pl.multiple_of(i * TM, TM)
                pltpu.make_async_copy(own_ref.at[:, pl.ds(r, TM), :], buf.at[slot], isem.at[slot]).start()

            @pl.when(i >= mine)
            def _():
                r = pl.multiple_of((i + shift) * TM, TM)
                pltpu.make_async_copy(sib_ref.at[:, pl.ds(r, TM), :], buf.at[slot], isem.at[slot]).start()

        def store(i, slot):
            for k in range(np_):
                if k == np_ - 1:
                    here, at = i >= keep, i - keep
                else:
                    here, at = jnp.logical_and(i >= starts[k], i < keep), i - starts[k]
                    if k + 1 < len(starts):
                        here = jnp.logical_and(here, i < starts[k + 1])

                @pl.when(here)
                def _():
                    r = pl.multiple_of(at * TM, TM)
                    pltpu.make_async_copy(buf.at[slot], outs[k].at[:, pl.ds(r, TM), :], osem.at[slot]).start()

        def stored(slot):
            pltpu.make_async_copy(buf.at[slot], outs[0].at[:, pl.ds(0, TM), :], osem.at[slot]).wait()

        for s in range(3):

            @pl.when(s < n)
            def _():
                load(s, s)

        def body(i, _):
            slot = lax.rem(i, 4)
            pltpu.make_async_copy(own_ref.at[:, pl.ds(0, TM), :], buf.at[slot], isem.at[slot]).wait()
            store(i, slot)

            @pl.when(i >= 1)
            def _():
                stored(lax.rem(i + 3, 4))

            @pl.when(i + 3 < n)
            def _():
                load(i + 3, lax.rem(i + 3, 4))

            return 0

        lax.fori_loop(0, n, body, 0)

        @pl.when(n > 0)
        def _():
            stored(lax.rem(n + 3, 4))

    return pl.pallas_call(
        kern,
        in_specs=[SM, ANY, ANY],
        out_specs=[ANY] * np_,
        out_shape=[jax.ShapeDtypeStruct((2, k * TM, D), BF) for k in sizes],
        scratch_shapes=[pltpu.VMEM((4, 2, TM, D), BF), pltpu.SemaphoreType.DMA((4,)), pltpu.SemaphoreType.DMA((4,))],
        compiler_params=pltpu.CompilerParams(vmem_limit_bytes=GRANT),
        cost_estimate=cost(10_000_000_000, 36_000_000),
        name="build_send",
    )(info, own, sib)


def append(tail, given, take):
    def kern(take_ref, tail_ref, given_ref, out_ref, buf, sem):
        for m in range(TAIL):

            @pl.when(m < take_ref[0])
            def _():
                src = given_ref.at[:, pl.ds(m * TM, TM), :]
                dst = out_ref.at[:, pl.ds((TAIL - 1 - m) * TM, TM), :]
                cp = pltpu.make_async_copy(src, buf, sem)
                cp.start()
                cp.wait()
                cp = pltpu.make_async_copy(buf, dst, sem)
                cp.start()
                cp.wait()

    return pl.pallas_call(
        kern,
        in_specs=[SM, ANY, ANY],
        out_specs=ANY,
        out_shape=jax.ShapeDtypeStruct((2, TAIL * TM, D), BF),
        scratch_shapes=[pltpu.VMEM((2, TM, D), BF), pltpu.SemaphoreType.DMA],
        input_output_aliases={1: 0},
        compiler_params=pltpu.CompilerParams(vmem_limit_bytes=GRANT),
        cost_estimate=cost(1_000_000_000, 4_000_000),
        name="append",
    )(take, tail, given)


def gelu_and_slope(u):
    u2 = u * u
    t = jnp.tanh(u * (C1 + (C1 * C3) * u2))
    half = 0.5 + 0.5 * t
    act = u * half
    slope = half + (0.5 * u) * (1.0 - t * t) * (C1 + (3 * C1 * C3) * u2)
    return act, slope


def pick(e, lo, hi, fn):
    if hi - lo == 1:
        fn(lo)
        return
    mid = (lo + hi) // 2

    @pl.when(e < mid * 32)
    def _():
        pick(e, lo, mid, fn)

    @pl.when(e >= mid * 32)
    def _():
        pick(e, mid, hi, fn)


def issue_group(tab_ref, g, slot, src, xb, db, sem):
    for s in range(G):
        e = tab_ref[g * G + s]
        r = pl.multiple_of(lax.rem(e, 32) * TM, TM)

        def fetch(k):
            rows = pl.ds(s * TM, TM)
            pltpu.make_async_copy(src[k].at[0, pl.ds(r, TM), :], xb.at[slot, rows, :], sem.at[slot, 0]).start()
            pltpu.make_async_copy(src[k].at[1, pl.ds(r, TM), :], db.at[slot, rows, :], sem.at[slot, 1]).start()

        pick(e, 0, len(src), fetch)


def wait_group(slot, xb, db, sem):
    pltpu.make_async_copy(xb.at[slot], xb.at[slot], sem.at[slot, 0]).wait()
    pltpu.make_async_copy(db.at[slot], db.at[slot], sem.at[slot, 1]).wait()


def add_group(x, dy, wu, wd, gd, gu):
    u = lax.dot_general(wu[...], x, (((0,), (1,)), ((), ())), preferred_element_type=F32).astype(BF).astype(F32)
    da = lax.dot_general(wd[...], dy, (((1,), (1,)), ((), ())), preferred_element_type=F32)
    act, slope = gelu_and_slope(u)
    dh = (da * slope).astype(BF)
    gd[...] += jnp.dot(act.astype(BF), dy, preferred_element_type=F32)
    gu[...] += jnp.dot(dh, x, preferred_element_type=F32)


def weight_copies(c, lo, at, w, wub, wdb, sem):
    w_up, sib, fx, fd, w_down, wd_oth = w
    y, f = at
    xi, core = f // 2, f % 2
    cps = []
    c0, co = c * HB, (c - lo) * HB
    if not isinstance(c, int):
        c0, co = pl.multiple_of(c0, HB), pl.multiple_of(co, HB)
    for a in range(2):
        xa = xi if a == 0 else 1 - xi
        col = pl.multiple_of(((2 * xa + core) * 2 + y) * HALF + c0, HB)
        parts = [w_up.at[:, pl.ds(col, HB)], sib.at[a, :, pl.ds(c0, HB)]]
        parts += [ref.at[a, :, pl.ds(co, HB)] for ref in (fx, fd)]
        for k, part in enumerate(parts):
            rows = pl.ds(pl.multiple_of((f ^ k) * 512, 512), 512)
            cps.append(pltpu.make_async_copy(part, wub.at[rows, pl.ds(a * HB, HB)], sem.at[k, a]))
    own = pl.ds(pl.multiple_of(y * HALF + c0, HB), HB)
    cps.append(pltpu.make_async_copy(w_down.at[own, :], wdb.at[pl.ds(0, HB), :], sem.at[4, 0]))
    cps.append(pltpu.make_async_copy(wd_oth.at[pl.ds(co, HB), :], wdb.at[pl.ds(HB, HB), :], sem.at[4, 1]))
    return cps


def gather_scratch(n_acc):
    return [
        pltpu.VMEM((2, M, D), BF),
        pltpu.VMEM((2, M, D), BF),
        pltpu.VMEM((n_acc, D, FB), BF),
        pltpu.VMEM((n_acc, FB, D), BF),
        pltpu.VMEM((n_acc, FB, D), F32),
        pltpu.VMEM((n_acc, FB, D), F32),
        pltpu.SemaphoreType.DMA((2, 2)),
        pltpu.SemaphoreType.DMA((n_acc, 5, 2)),
    ]


def early_grads(tab, info, srcs, wsets, lo_chunk, n_new, prior=(), deps=()):
    ns, nw, npr = len(srcs), len(wsets), len(prior)
    sizes = [p[0].shape[0] for p in prior]
    n_chunks = n_new + sum(sizes)

    def kern(tab_ref, info_ref, *refs):
        src, refs = refs[:ns], refs[ns:]
        wrefs, refs = [refs[6 * k : 6 * k + 6] for k in range(nw)], refs[6 * nw :]
        pri, refs = refs[: 2 * npr], refs[2 * npr + len(deps) :]
        out_d, out_u, xb, db, wub, wdb, gd, gu, sem, wsem, asem = refs
        hi, at = info_ref[1], (info_ref[2], info_ref[3])

        def lo(q):
            return jnp.where(q < n_new, 0, info_ref[0])

        def weights(q, slot, act):
            c = jnp.where(q < n_new, lo_chunk + q, q - n_new) if npr else lo_chunk + q

            def act_all(k):
                for cp in weight_copies(c, wsets[k][0], at, wrefs[k], wub.at[slot], wdb.at[slot], wsem.at[slot]):
                    act(cp)

            if nw == 1:
                act_all(0)
                return
            for k in range(nw):
                first, count, _ = wsets[k]

                @pl.when(jnp.logical_and(c >= first, c < first + count))
                def _():
                    act_all(k)

        def start_copy(cp):
            cp.start()

        def wait_copy(cp):
            cp.wait()

        def results(q, slot):
            return (
                pltpu.make_async_copy(gd.at[slot], out_d.at[q], asem.at[slot, 0]),
                pltpu.make_async_copy(gu.at[slot], out_u.at[q], asem.at[slot, 1]),
            )

        issue_group(tab_ref, lo(0), 0, src, xb, db, sem)
        weights(0, 0, start_copy)

        def chunk(q, t):
            ws = lax.rem(q, 2)

            @pl.when(q + 1 < n_chunks)
            def _():
                weights(q + 1, 1 - ws, start_copy)

            @pl.when(q >= 2)
            def _():
                for cp in results(q - 2, ws):
                    cp.wait()

            @pl.when(q < n_new)
            def _():
                gd[ws] = jnp.zeros((FB, D), F32)
                gu[ws] = jnp.zeros((FB, D), F32)

            base = n_new
            for k in range(npr):
                first, base = base, base + sizes[k]

                @pl.when(jnp.logical_and(q >= first, q < base))
                def _():
                    cps = (
                        pltpu.make_async_copy(pri[2 * k].at[q - first], gd.at[ws], asem.at[ws, 0]),
                        pltpu.make_async_copy(pri[2 * k + 1].at[q - first], gu.at[ws], asem.at[ws, 1]),
                    )
                    for cp in cps:
                        cp.start()
                    for cp in cps:
                        cp.wait()

            weights(q, ws, wait_copy)

            def group(g, t):
                slot = lax.rem(t, 2)
                last = g + 1 == hi

                @pl.when(jnp.logical_or(jnp.logical_not(last), q + 1 < n_chunks))
                def _():
                    issue_group(tab_ref, jnp.where(last, lo(q + 1), g + 1), 1 - slot, src, xb, db, sem)

                wait_group(slot, xb, db, sem)
                add_group(xb[slot], db[slot], wub.at[ws], wdb.at[ws], gd.at[ws], gu.at[ws])
                return t + 1

            t = lax.fori_loop(lo(q), hi, group, t)
            for cp in results(q, ws):
                cp.start()
            return t

        lax.fori_loop(0, n_chunks, chunk, 0)
        for q in range(max(n_chunks - 2, 0), n_chunks):
            for cp in results(q, q % 2):
                cp.wait()

    flat = [a for _, _, w in wsets for a in w]
    pri = [a for p in prior for a in p]
    return pl.pallas_call(
        kern,
        in_specs=[SM, SM] + [ANY] * (ns + len(flat) + len(pri)) + [SM] * len(deps),
        out_specs=[ANY] * 2,
        out_shape=[jax.ShapeDtypeStruct((n_chunks, FB, D), F32)] * 2,
        scratch_shapes=gather_scratch(2) + [pltpu.SemaphoreType.DMA((2, 2))],
        compiler_params=pltpu.CompilerParams(vmem_limit_bytes=GRANT),
        cost_estimate=cost(8 * 5632 * D * FB * n_new, 60_000_000 * n_new),
    )(tab, info, *srcs, *flat, *pri, *deps)


def chunk_grads(j, tab, info, srcs, wset, prior, at, deps):
    ns = len(srcs)
    w_lo, _, w = wset

    def kern(tab_ref, info_ref, *refs):
        src, refs = refs[:ns], refs[ns:]
        wrefs, (pd, pu), refs = refs[:6], refs[6:8], refs[8 + len(deps) :]
        keep_d, send_d, keep_u, send_u, xb, db, wub, wdb, gd, gu, sem, wsem, osem = refs
        groups, y, f = info_ref[0], info_ref[1], info_ref[2]
        xi = f // 2
        wub, wdb, gd, gu = wub.at[0], wdb.at[0], gd.at[0], gu.at[0]

        @pl.when(groups > 0)
        def _():
            issue_group(tab_ref, 0, 0, src, xb, db, sem)

        cps = weight_copies(j, w_lo, (y, f), wrefs, wub, wdb, wsem.at[0])
        cps.append(pltpu.make_async_copy(pd.at[at], gd, osem.at[0]))
        cps.append(pltpu.make_async_copy(pu.at[at], gu, osem.at[1]))
        for cp in cps:
            cp.start()
        for cp in cps:
            cp.wait()

        def body(g, _):
            slot = lax.rem(g, 2)

            @pl.when(g + 1 < groups)
            def _():
                issue_group(tab_ref, g + 1, 1 - slot, src, xb, db, sem)

            wait_group(slot, xb, db, sem)
            add_group(xb[slot], db[slot], wub, wdb, gd, gu)
            return 0

        lax.fori_loop(0, groups, body, 0)
        kc = pl.multiple_of(xi * HALF, HALF)
        sc = pl.multiple_of((1 - xi) * HALF, HALF)
        ocp = [(gd.at[pl.ds(HB, HB), :], send_d), (gd.at[pl.ds(0, HB), :], keep_d)]
        for a in range(2):
            rows, cols = pl.ds(a * HB, HB), pl.ds(a * HALF, HALF)
            ocp.append((gu.at[rows, pl.ds(sc, HALF)], send_u.at[:, cols]))
            ocp.append((gu.at[rows, pl.ds(kc, HALF)], keep_u.at[:, cols]))
        ocp = [pltpu.make_async_copy(a, b, osem.at[i]) for i, (a, b) in enumerate(ocp)]
        for cp in ocp:
            cp.start()
        for cp in ocp:
            cp.wait()

    return pl.pallas_call(
        kern,
        in_specs=[SM, SM] + [ANY] * (ns + 8 + len(deps)),
        out_specs=[ANY] * 4,
        out_shape=[jax.ShapeDtypeStruct((HB, D), F32)] * 4,
        scratch_shapes=gather_scratch(1) + [pltpu.SemaphoreType.DMA((6,))],
        compiler_params=pltpu.CompilerParams(vmem_limit_bytes=GRANT),
        cost_estimate=cost(8 * 3072 * D * FB, 40_000_000),
    )(tab, info, *srcs, *w, *prior, *deps)


def finish_down(j, pos, keep, recv, out):
    first = out is None

    def kern(pos_ref, kd, rc, *refs):
        out_d, fd, vd, sem = refs if first else refs[1:]
        y = pos_ref[0]
        vd[...] = kd[...] + rc[...]
        row = pl.multiple_of(y * HALF + j * HB, HB)
        cps = [
            pltpu.make_async_copy(vd, fd, sem.at[0]),
            pltpu.make_async_copy(vd, out_d.at[pl.ds(row, HB), :], sem.at[1]),
        ]
        for cp in cps:
            cp.start()
        for cp in cps:
            cp.wait()

    extra = [] if first else [out]
    return pl.pallas_call(
        kern,
        in_specs=[SM, VM, VM] + [ANY] * len(extra),
        out_specs=[ANY] * 2,
        out_shape=[jax.ShapeDtypeStruct((D, D), F32), jax.ShapeDtypeStruct((HB, D), F32)],
        scratch_shapes=[pltpu.VMEM((HB, D), F32), pltpu.SemaphoreType.DMA((2,))],
        input_output_aliases={} if first else {3: 0},
        compiler_params=pltpu.CompilerParams(vmem_limit_bytes=GRANT),
        cost_estimate=cost(2_000_000_000, 4_000_000),
    )(pos, keep, recv, *extra)


def finish_up(j, pos, keep, recv, out):
    first = out is None

    def kern(pos_ref, ku, rc, *refs):
        out_u, fuc, fus, vu, sem = refs if first else refs[1:]
        y, xi, c = pos_ref[0], pos_ref[1], pos_ref[2]
        mine = pl.ds(pl.multiple_of(c * 512, 512), 512)
        other = pl.ds(pl.multiple_of((1 - c) * 512, 512), 512)
        vu[0] = (ku[:, 0:HALF] + rc[:, HALF:D]).T
        vu[1] = (ku[:, HALF:D] + rc[:, 0:HALF]).T
        cps = [
            pltpu.make_async_copy(vu.at[:, other, :], fus, sem.at[0]),
            pltpu.make_async_copy(vu.at[:, mine, :], fuc, sem.at[1]),
        ]
        for a in range(2):
            xa = xi if a == 0 else 1 - xi
            col = pl.multiple_of(((2 * xa + c) * 2 + y) * HALF + j * HB, HB)
            cps.append(pltpu.make_async_copy(vu.at[a, mine, :], out_u.at[:, pl.ds(col, HB)], sem.at[2 + a]))
        for cp in cps:
            cp.start()
        for cp in cps:
            cp.wait()

    extra = [] if first else [out]
    return pl.pallas_call(
        kern,
        in_specs=[SM, VM, VM] + [ANY] * len(extra),
        out_specs=[ANY] * 3,
        out_shape=[
            jax.ShapeDtypeStruct((512, 4 * D), F32),
            jax.ShapeDtypeStruct((2, 512, HB), F32),
            jax.ShapeDtypeStruct((2, 512, HB), F32),
        ],
        scratch_shapes=[pltpu.VMEM((2, HALF, HB), F32), pltpu.SemaphoreType.DMA((4,))],
        input_output_aliases={} if first else {3: 0},
        compiler_params=pltpu.CompilerParams(vmem_limit_bytes=GRANT),
        cost_estimate=cost(2_000_000_000, 4_000_000),
    )(pos, keep, recv, *extra)


def store(j, pos, rd, ruc, ruy, rus, outs):
    def kern(pos_ref, d_ref, uc_ref, uy_ref, us_ref, _d, _u, out_d, out_u, vd, vu, isem, osem):
        y, xi, c = pos_ref[0], pos_ref[1], pos_ref[2]
        row = pl.multiple_of((1 - y) * HALF + j * HB, HB)
        work = [(d_ref, vd, [(vd, out_d.at[pl.ds(row, HB), :])])]
        for k, (ref, cc, yy) in enumerate(((uc_ref, c, 1 - y), (uy_ref, 1 - c, 1 - y), (us_ref, 1 - c, y))):
            puts = []
            for a in range(2):
                xa = xi if a == 0 else 1 - xi
                col = pl.multiple_of(((2 * xa + cc) * 2 + yy) * HALF + j * HB, HB)
                puts.append((vu.at[k, a], out_u.at[:, pl.ds(col, HB)]))
            work.append((ref, vu.at[k], puts))
        loads = [pltpu.make_async_copy(src, mid, isem.at[n]) for n, (src, mid, _) in enumerate(work)]
        for cp in loads:
            cp.start()
        done = []
        for cp, (_, _, puts) in zip(loads, work):
            cp.wait()
            for src, dst in puts:
                put = pltpu.make_async_copy(src, dst, osem.at[len(done)])
                put.start()
                done.append(put)
        for put in done:
            put.wait()

    return pl.pallas_call(
        kern,
        in_specs=[SM] + [ANY] * 6,
        out_specs=[ANY] * 2,
        out_shape=[jax.ShapeDtypeStruct((D, D), F32), jax.ShapeDtypeStruct((512, 4 * D), F32)],
        scratch_shapes=[
            pltpu.VMEM((HB, D), F32),
            pltpu.VMEM((3, 2, 512, HB), F32),
            pltpu.SemaphoreType.DMA((4,)),
            pltpu.SemaphoreType.DMA((7,)),
        ],
        input_output_aliases={5: 0, 6: 1},
        compiler_params=pltpu.CompilerParams(vmem_limit_bytes=16 * MIB),
        cost_estimate=cost(3_000_000_000, 5_000_000),
    )(pos, rd, ruc, ruy, rus, *outs)


def nothing(k):
    return pl.pallas_call(lambda o: None, out_specs=ANY, out_shape=jax.ShapeDtypeStruct((2, k * TM, D), BF))()


def exchange_branch(parts, early):
    here = [k in parts for k in range(len(MAIN))]

    def run(pieces, tail, give, take, *rest):
        got = []
        for k in range(len(MAIN)):
            got.append(y_swap(pieces[k]) if here[k] else nothing(MAIN[k]))
        given = x_swap(give)
        acc = early(0, *rest)
        given_s = core_swap(given)
        tail = append(tail, given, take)
        last = y_swap(tail)
        acc = (*acc, *early(1, *rest))
        sib = []
        for k in range(len(MAIN)):
            sib.append(core_swap(got[k]) if here[k] else nothing(MAIN[k]))
        last_s = core_swap(last)
        return (*got, last, *sib, last_s, given, given_s, *acc)

    return run


def piece_starts():
    table = []
    for size, parts in zip(SIZES, PARTS):
        at, row = FIRST, []
        for k in range(len(MAIN)):
            row.append(at)
            at += MAIN[k] if k in parts else 0
        assert at + TAIL == FIRST + size
        table.append([*row, at])
    return table


def solution(mesh):
    tok_spec = P(None, ("model", "replica", "fsdp"), None)
    len_spec = P(None, ("model", "replica", "fsdp"))
    w_spec = P(None, ("model", "fsdp"), None)

    def group_grads(x_in, dy, lengths, w_up, w_down):
        y, f = lax.axis_index("replica"), lax.axis_index("fsdp")
        xi, c = f // 2, f % 2
        w_up, w_down = w_up[0], w_down[0]

        row = jnp.zeros((8, 128), jnp.int32).at[:MICRO, 0].set(lengths[:, 0].astype(jnp.int32))
        around, s1 = start(row, x_in, dy)
        s1 = s1.reshape(2, MICRO * BASE, D)
        s1_y = y_swap(s1)
        me = y * 4 + f
        lens = around[(me - jnp.arange(8)) % 8][:, :MICRO, 0]

        def cols(xd, cd, lo=0, n=HALF):
            own = lax.dynamic_slice(w_up, (0, ((2 * xd + cd) * 2 + y) * HALF + lo), (512, n))
            oth = lax.dynamic_slice(w_up, (0, ((2 * (1 - xd) + cd) * 2 + y) * HALF + lo), (512, n))
            return jnp.stack([own, oth])

        from_s = core_swap(cols(xi, 1 - c))
        wsets = []
        for lo, n in WSETS:
            a = x_swap(cols(1 - xi, c, lo * HB, n * HB))
            b = x_diag(cols(1 - xi, 1 - c, lo * HB, n * HB))
            d = x_swap(lax.dynamic_slice(w_down, (y * HALF + lo * HB, 0), (n * HB, D)))
            wsets.append((lo, n, [w_up, from_s, a, b, w_down, d]))

        rest = lens - BASE
        r16 = (rest + 15) // 16 * 16
        tiles = (jnp.sum(r16, axis=1) + TM - 1) // TM
        my_rest = lax.dynamic_index_in_dim(rest, me, keepdims=False)
        my16 = lax.dynamic_index_in_dim(r16, me, keepdims=False)
        offs = jnp.concatenate([jnp.zeros((1,), jnp.int32), jnp.cumsum(my16)])
        both = tiles[0::2] + tiles[1::2]
        share = jnp.stack([(both + 1) // 2, both // 2], axis=1).reshape(8)
        gap = share - share[jnp.arange(8) ^ 2]
        move = jnp.minimum(jnp.abs(gap) // 2, TAIL)
        keep = share - jnp.where(gap > 0, move, 0)
        take = jnp.where(gap < 0, move, 0)
        which = jnp.sum(jnp.max(keep + take) - FIRST > jnp.array(SIZES[:-1]))
        starts = jnp.array(piece_starts())[which]
        end = starts[-1] + TAIL

        def at(v, i):
            return lax.dynamic_index_in_dim(v, i, keepdims=False)

        t_own, t_sib = at(tiles, me), at(tiles, me ^ 1)
        h_own, h_sib = at(share, me), at(share, me ^ 1)
        k_own, k_sib, k_y, k_ys = (at(keep, me ^ k) for k in (0, 1, 4, 5))
        x_own, x_sib, x_y, x_ys = (at(take, me ^ k) for k in (0, 1, 4, 5))

        packed = pack_rest(x_in, dy, my_rest, offs)
        packed_s = core_swap(packed)
        s1_s = core_swap(s1)
        pa, *pieces, tail, give = build_send(
            packed, packed_s,
            jnp.concatenate([jnp.stack([h_own, k_own, t_own, t_sib - h_own]), starts]).astype(jnp.int32),
        )
        qa = y_swap(pa)

        i = jnp.arange(64)
        n_own = 12 + k_own + k_sib
        g_own = (n_own + G - 1) // G
        k = i - g_own * G
        m, n = i - 12, i - 12 - k_own
        tab = jnp.where(n < t_sib, 3 * 32 + n, 2 * 32 + n + t_own - h_sib)
        tab = jnp.where(n < 0, jnp.where(m < t_own, 2 * 32 + m, 3 * 32 + m + t_sib - h_own), tab)
        tab = jnp.where(i < n_own, tab, 2 * 32 + NT)
        tab = jnp.where(i < 12, (i // 6) * 32 + i % 6, tab)
        tab = jnp.where((k >= 0) & (k < 12), (4 + k // 6) * 32 + k % 6, tab).astype(jnp.int32)
        info_own = jnp.stack([0, g_own, y, f]).astype(jnp.int32)
        info_all = jnp.stack([g_own, g_own + 3, y, f]).astype(jnp.int32)

        n_src = 2 + len(MAIN)
        l_y, l_ys = k_y + x_y, k_ys + x_ys
        i = jnp.arange(48)
        first = i < l_y
        t = jnp.where(first, i, i - l_y)
        listed = jnp.where(first, k_y, k_ys)
        t = jnp.where(t < listed, t, end - 1 - (t - listed))
        late = t
        for n in range(n_src - 1):
            late = jnp.where(t >= starts[n], (1 + n) * 32 + t - starts[n], late)
        late = jnp.where(first, late, late + n_src * 32)
        m = i - l_y - l_ys
        handed = jnp.where(m < x_own, 2 * n_src * 32 + m, (2 * n_src + 1) * 32 + m - x_own)
        late = jnp.where(m < 0, late, jnp.where(m < x_own + x_sib, handed, (2 * n_src + 2) * 32 + NT)).astype(jnp.int32)
        info_late = jnp.stack([(l_y + l_ys + x_own + x_sib + G - 1) // G, y, f]).astype(jnp.int32)
        pos = jnp.stack([y, xi, c]).astype(jnp.int32)

        own_srcs = (s1, s1_s, packed, packed_s)
        acc0 = early_grads(tab, info_own, own_srcs, wsets[:1], 0, 2)
        acc1 = early_grads(tab, info_own, own_srcs, wsets[1:2], 2, 1, (), (late, info_late, pos))
        s1_ys = core_swap(s1_y)
        srcs = (*own_srcs, s1_y, s1_ys)

        def early(step, tab, info, srcs, w, prior):
            sets = [(lo, n, v) for (lo, n), v in zip(WSETS, w)]
            if step == 0:
                return early_grads(tab, info, srcs, sets[1:], 3, 2)
            return early_grads(tab, info, srcs, sets, 5, 3, prior)

        got = lax.switch(
            which,
            [exchange_branch(parts, early) for parts in PARTS],
            pieces, tail, give, x_own.reshape(1).astype(jnp.int32),
            tab, info_all, srcs, [w for _, _, w in wsets], [list(acc0), list(acc1)],
        )
        k = len(MAIN) + 1
        pieces, sib_pieces, given, acc3, acc4 = got[:k], got[k : 2 * k], got[2 * k : 2 * k + 2], got[-4:-2], got[-2:]
        qas = core_swap(qa)
        srcs = (qa, *pieces, qas, *sib_pieces, *given, packed)
        prior = [(acc4, 3), (acc4, 4), (acc4, 5), (acc3, 0), (acc3, 1), (acc4, 0), (acc4, 1), (acc4, 2)]

        out_d = out_u = None
        fin = []
        for p, j in enumerate(ORDER):
            deps = (fin[p - 2][0],) if p >= 2 else ()
            w_at = next(h for h, (lo, n) in enumerate(WSETS) if lo <= j < lo + n)
            keep_d, send_d, keep_u, send_u = chunk_grads(
                j, late, info_late, srcs, wsets[w_at], *prior[j], deps
            )
            recv_d = x_swap(send_d)
            recv_u = x_swap(send_u)
            out_d, fd = finish_down(j, pos, keep_d, recv_d, out_d)
            rd = y_swap(fd)
            out_u, fuc, fus = finish_up(j, pos, keep_u, recv_u, out_u)
            ruc = y_swap(fuc)
            ruy = y_diag(fus)
            rus = core_swap(fus)
            fin.append((fd, (rd, ruc, ruy, rus)))
            if p >= LAG:
                out_d, out_u = store(ORDER[p - LAG], pos, *fin[p - LAG][1], (out_d, out_u))
        for p in range(NCH - LAG, NCH):
            out_d, out_u = store(ORDER[p], pos, *fin[p][1], (out_d, out_u))
        return out_u[None], out_d[None]


    return jax.shard_map(
        group_grads,
        mesh=mesh,
        in_specs=(tok_spec, tok_spec, len_spec, w_spec, w_spec),
        out_specs=(w_spec, w_spec),
        check_vma=False,
    )
```

```python
import jax
import jax.numpy as jnp
from jax import lax
from jax.experimental import pallas as pl
from jax.experimental.pallas import tpu as pltpu
from jax.sharding import PartitionSpec as P


D = 2048
TOK = 1024
MICRO = 3
BASE = 256
REST = TOK - BASE
TM = 128
NT = MICRO * REST // TM
RROWS = MICRO * REST + TM
FIRST = 3
MAIN = (4, 4, 3, 2)
TAIL = 2
SIZES = (15, 12, 6, 11, 10, 7, 9, 8)
PARTS = ((0, 1, 2, 3), (0, 1, 3), (0,), (0, 2, 3), (0, 1), (2, 3), (0, 2), (0, 3))
N_TAB, N_LATE = 64, 48
G = 4
M = G * TM
FB = 256
HB = FB // 2
NCH = D // FB
HALF = 1024
WSETS = ((0, 2), (2, 2), (4, 4))
ORDER = (3, 4, 0, 5, 6, 1, 7, 2)
LAG = 3
C1 = 0.7978845608028654
C3 = 0.044715
BF = jnp.bfloat16
F32 = jnp.float32


ANY = pl.BlockSpec(memory_space=pltpu.HBM)
SM = pl.BlockSpec(memory_space=pltpu.SMEM)
VM = pl.BlockSpec(memory_space=pltpu.VMEM)
MIB = 1024 * 1024
GRANT = 60 * 1024 * 1024

CORE = [(0, 1), (1, 0), (2, 3), (3, 2)]
XSWAP = [(0, 2), (2, 0), (1, 3), (3, 1)]
XDIAG = [(0, 3), (3, 0), (1, 2), (2, 1)]
YSWAP = [(0, 1), (1, 0)]
YDIAG = [(r * 4 + f, (1 - r) * 4 + (f ^ 1)) for r in range(2) for f in range(4)]


def core_swap(v):
    return lax.ppermute(v, "fsdp", CORE)


def x_swap(v):
    return lax.ppermute(v, "fsdp", XSWAP)


def x_diag(v):
    return lax.ppermute(v, "fsdp", XDIAG)


def y_swap(v):
    return lax.ppermute(v, "replica", YSWAP)


def y_diag(v):
    return lax.ppermute(v, ("replica", "fsdp"), YDIAG)


def cost(flops, nbytes):
    return pl.CostEstimate(flops=flops, bytes_accessed=nbytes, transcendentals=0)


def start(lens, x_in, dy):
    def kern(len_ref, x_ref, d_ref, all_ref, s1_ref, land, buf, send, recv, isem, osem):
        r, f = lax.axis_index("replica"), lax.axis_index("fsdp")
        me = r * 4 + f
        loads = []
        for a, ref in enumerate((x_ref, d_ref)):
            cp = pltpu.make_async_copy(ref.at[:, pl.ds(0, BASE), :], buf.at[a], isem.at[a])
            cp.start()
            loads.append(cp)
        barrier = pltpu.get_barrier_semaphore()
        peers = []
        for k in range(1, 8):
            p = lax.rem(me + k, 8)
            peers.append((0, p // 4, lax.rem(p, 4)))
        for p in peers:
            pl.semaphore_signal(barrier, inc=1, device_id=p, device_id_type=pl.DeviceIdType.MESH)
        pl.semaphore_wait(barrier, 7)
        cps = []
        for k, p in enumerate(peers):
            cp = pltpu.make_async_remote_copy(
                src_ref=len_ref,
                dst_ref=land.at[k],
                send_sem=send.at[k],
                recv_sem=recv.at[k],
                device_id=p,
                device_id_type=pl.DeviceIdType.MESH,
            )
            cp.start()
            cps.append(cp)
        outs = []
        for a in range(2):
            loads[a].wait()
            cp = pltpu.make_async_copy(buf.at[a], s1_ref.at[a], osem.at[a])
            cp.start()
            outs.append(cp)
        for cp in cps:
            cp.wait()
        all_ref[0:1, :] = len_ref[0:1, :]
        for k in range(7):
            all_ref[k + 1 : k + 2, :] = land[k, 0:1, :]
        for cp in outs:
            cp.wait()

    return pl.pallas_call(
        kern,
        in_specs=[VM, ANY, ANY],
        out_specs=[VM, ANY],
        out_shape=[jax.ShapeDtypeStruct((8, 128), jnp.int32), jax.ShapeDtypeStruct((2, MICRO, BASE, D), BF)],
        scratch_shapes=[
            pltpu.VMEM((7, 8, 128), jnp.int32),
            pltpu.VMEM((2, MICRO, BASE, D), BF),
            pltpu.SemaphoreType.DMA((7,)),
            pltpu.SemaphoreType.DMA((7,)),
            pltpu.SemaphoreType.DMA((2,)),
            pltpu.SemaphoreType.DMA((2,)),
        ],
        compiler_params=pltpu.CompilerParams(collective_id=0, has_side_effects=True, vmem_limit_bytes=GRANT),
        cost_estimate=cost(10_000_000_000, 13_000_000),
        name="start",
    )(lens, x_in, dy)


def plan(around):
    names = dict(
        rest=MICRO, offs=MICRO + 1, send=4 + len(MAIN) + 1, take=1, which=1, tab=N_TAB, own=4, every=4, late=N_LATE,
        info=3, pos=3,
    )

    def kern(all_ref, rest_ref, offs_ref, send_ref, take_ref, which_ref, tab_ref, own_ref, every_ref, late_ref, info_ref,
             pos_ref):
        y, f = lax.axis_index("replica"), lax.axis_index("fsdp")
        xi, c = f // 2, lax.rem(f, 2)
        me = y * 4 + f

        def at(values, i):
            return sum(jnp.where(i == d, v, 0) for d, v in enumerate(values))

        o = jnp.int32(0)
        for k in range(MICRO):
            n = all_ref[0, k] - BASE
            rest_ref[k], offs_ref[k] = n, o
            o = o + (n + 15) // 16 * 16
        offs_ref[MICRO] = o
        tiles = []
        for d in range(8):
            row = lax.rem(me - d + 8, 8)
            n = sum((all_ref[row, k] - BASE + 15) // 16 * 16 for k in range(MICRO))
            tiles.append((n + TM - 1) // TM)
        share = []
        for q in range(4):
            both = tiles[2 * q] + tiles[2 * q + 1]
            share += [(both + 1) // 2, both // 2]
        keep, take = [], []
        for d in range(8):
            gap = share[d] - share[d ^ 2]
            move = jnp.minimum(jnp.abs(gap) // 2, TAIL)
            keep.append(share[d] - jnp.where(gap > 0, move, 0))
            take.append(jnp.where(gap < 0, move, 0))
        longest = keep[0] + take[0]
        for d in range(1, 8):
            longest = jnp.maximum(longest, keep[d] + take[d])
        order = sorted(range(len(SIZES)), key=lambda k: SIZES[k])
        rank = sum(jnp.where(longest - FIRST > SIZES[k], 1, 0) for k in order[:-1])
        which = at(order, rank)
        table = piece_starts()
        starts = [at([row[k] for row in table], which) for k in range(len(MAIN) + 1)]
        end = starts[-1] + TAIL
        t_own, t_sib = at(tiles, me), at(tiles, me ^ 1)
        h_own, h_sib = at(share, me), at(share, me ^ 1)
        k_own, k_sib, k_y, k_ys = (at(keep, me ^ k) for k in (0, 1, 4, 5))
        x_own, x_sib, x_y, x_ys = (at(take, me ^ k) for k in (0, 1, 4, 5))
        for k, v in enumerate((h_own, k_own, t_own, t_sib - h_own, *starts)):
            send_ref[k] = v
        take_ref[0], which_ref[0] = x_own, which

        n_own = 12 + k_own + k_sib
        g_own = (n_own + G - 1) // G

        def early_entry(i, _):
            k, m, n = i - g_own * G, i - 12, i - 12 - k_own
            e = jnp.where(n < t_sib, 3 * 32 + n, 2 * 32 + n + t_own - h_sib)
            e = jnp.where(n < 0, jnp.where(m < t_own, 2 * 32 + m, 3 * 32 + m + t_sib - h_own), e)
            e = jnp.where(i < n_own, e, 2 * 32 + NT)
            e = jnp.where(i < 6, i, jnp.where(i < 12, 32 + i - 6, e))
            e = jnp.where(k >= 0, jnp.where(k < 6, 4 * 32 + k, 5 * 32 + k - 6), e)
            tab_ref[i] = jnp.where(k >= 12, 2 * 32 + NT, e)
            return 0

        lax.fori_loop(0, N_TAB, early_entry, 0)
        for k, (a, b) in enumerate(((0, g_own), (g_own, g_own + 3), (y, y), (f, f))):
            own_ref[k], every_ref[k] = a, b

        n_src = 2 + len(MAIN)
        l_y, l_ys = k_y + x_y, k_ys + x_ys

        def late_entry(i, _):
            first = i < l_y
            t = jnp.where(first, i, i - l_y)
            listed = jnp.where(first, k_y, k_ys)
            t = jnp.where(t < listed, t, end - 1 - (t - listed))
            e = t
            for n in range(n_src - 1):
                e = jnp.where(t >= starts[n], (1 + n) * 32 + t - starts[n], e)
            e = jnp.where(first, e, e + n_src * 32)
            m = i - l_y - l_ys
            handed = jnp.where(m < x_own, 2 * n_src * 32 + m, (2 * n_src + 1) * 32 + m - x_own)
            late_ref[i] = jnp.where(m < 0, e, jnp.where(m < x_own + x_sib, handed, (2 * n_src + 2) * 32 + NT))
            return 0

        lax.fori_loop(0, N_LATE, late_entry, 0)
        for k, v in enumerate(((l_y + l_ys + x_own + x_sib + G - 1) // G, y, f)):
            info_ref[k] = v
        for k, v in enumerate((y, xi, c)):
            pos_ref[k] = v

    outs = pl.pallas_call(
        kern,
        in_specs=[SM],
        out_specs=[SM] * len(names),
        out_shape=[jax.ShapeDtypeStruct((n,), jnp.int32) for n in names.values()],
        cost_estimate=cost(3_000_000_000, 10_000),
        name="plan",
    )(around)
    return dict(zip(names, outs))


def pack_rest(x_in, dy, rest, offs):
    per = REST // TM

    def kern(rest_ref, offs_ref, x_ref, d_ref, out_ref, buf, zero, isem, osem, zsem):
        def load(k, t):
            rows = pl.ds(BASE + t * TM, TM)
            return [
                pltpu.make_async_copy(ref.at[k, rows, :], buf.at[k, t, a], isem.at[k, t, a])
                for a, ref in enumerate((x_ref, d_ref))
            ]

        def put(k, t):
            o = pl.multiple_of(offs_ref[k] + t * TM, 16)
            return [
                pltpu.make_async_copy(buf.at[k, t, a], out_ref.at[a, pl.ds(o, TM), :], osem.at[t, a]) for a in range(2)
            ]

        def each(k, fn):
            for t in range(per):

                @pl.when(t * TM < rest_ref[k])
                def _():
                    fn(k, t)

        def begin(k, t):
            for cp in load(k, t):
                cp.start()

        def move(k, t):
            for cp in load(k, t):
                cp.wait()
            n = rest_ref[k] - t * TM

            @pl.when(n < TM)
            def _():
                ragged = pl.multiple_of(n // 16 * 16, 16)
                row = lax.broadcasted_iota(jnp.int32, (16, D), 0) + ragged
                blk = buf[k, t, 1, pl.ds(ragged, 16), :]
                buf[k, t, 1, pl.ds(ragged, 16), :] = jnp.where(row < n, blk, jnp.zeros_like(blk))

            for cp in put(k, t):
                cp.start()

        def end(k, t):
            for cp in put(k, t):
                cp.wait()

        for k in range(MICRO):
            each(k, begin)
        zero[...] = jnp.zeros_like(zero)
        for k in range(MICRO):
            each(k, move)
            each(k, end)
        for o in (pl.multiple_of(offs_ref[MICRO], 16), MICRO * REST):
            cps = [pltpu.make_async_copy(zero, out_ref.at[a, pl.ds(o, TM), :], zsem.at[a]) for a in range(2)]
            for cp in cps:
                cp.start()
            for cp in cps:
                cp.wait()

    return pl.pallas_call(
        kern,
        in_specs=[SM, SM, ANY, ANY],
        out_specs=ANY,
        out_shape=jax.ShapeDtypeStruct((2, RROWS, D), BF),
        scratch_shapes=[
            pltpu.VMEM((MICRO, per, 2, TM, D), BF),
            pltpu.VMEM((TM, D), BF),
            pltpu.SemaphoreType.DMA((MICRO, per, 2)),
            pltpu.SemaphoreType.DMA((per, 2)),
            pltpu.SemaphoreType.DMA((2,)),
        ],
        compiler_params=pltpu.CompilerParams(vmem_limit_bytes=GRANT),
        cost_estimate=cost(15_000_000_000, 50_000_000),
        name="pack_rest",
    )(rest, offs, x_in, dy)


def build_send(own, sib, info):
    sizes = (FIRST, *MAIN, TAIL, TAIL)
    np_ = len(sizes)

    def kern(info_ref, own_ref, sib_ref, *refs):
        outs, (buf, isem, osem) = refs[:np_], refs[np_:]
        n, keep, mine, shift = info_ref[0], info_ref[1], info_ref[2], info_ref[3]
        starts = [0] + [info_ref[4 + k] for k in range(np_ - 2)]

        def load(i, slot):
            @pl.when(i < mine)
            def _():
                r = pl.multiple_of(i * TM, TM)
                pltpu.make_async_copy(own_ref.at[:, pl.ds(r, TM), :], buf.at[slot], isem.at[slot]).start()

            @pl.when(i >= mine)
            def _():
                r = pl.multiple_of((i + shift) * TM, TM)
                pltpu.make_async_copy(sib_ref.at[:, pl.ds(r, TM), :], buf.at[slot], isem.at[slot]).start()

        def store(i, slot):
            for k in range(np_):
                if k == np_ - 1:
                    here, at = i >= keep, i - keep
                else:
                    here, at = jnp.logical_and(i >= starts[k], i < keep), i - starts[k]
                    if k + 1 < len(starts):
                        here = jnp.logical_and(here, i < starts[k + 1])

                @pl.when(here)
                def _():
                    r = pl.multiple_of(at * TM, TM)
                    pltpu.make_async_copy(buf.at[slot], outs[k].at[:, pl.ds(r, TM), :], osem.at[slot]).start()

        def stored(slot):
            pltpu.make_async_copy(buf.at[slot], outs[0].at[:, pl.ds(0, TM), :], osem.at[slot]).wait()

        for s in range(3):

            @pl.when(s < n)
            def _():
                load(s, s)

        def body(i, _):
            slot = lax.rem(i, 4)
            pltpu.make_async_copy(own_ref.at[:, pl.ds(0, TM), :], buf.at[slot], isem.at[slot]).wait()
            store(i, slot)

            @pl.when(i >= 1)
            def _():
                stored(lax.rem(i + 3, 4))

            @pl.when(i + 3 < n)
            def _():
                load(i + 3, lax.rem(i + 3, 4))

            return 0

        lax.fori_loop(0, n, body, 0)

        @pl.when(n > 0)
        def _():
            stored(lax.rem(n + 3, 4))

    return pl.pallas_call(
        kern,
        in_specs=[SM, ANY, ANY],
        out_specs=[ANY] * np_,
        out_shape=[jax.ShapeDtypeStruct((2, k * TM, D), BF) for k in sizes],
        scratch_shapes=[pltpu.VMEM((4, 2, TM, D), BF), pltpu.SemaphoreType.DMA((4,)), pltpu.SemaphoreType.DMA((4,))],
        compiler_params=pltpu.CompilerParams(vmem_limit_bytes=GRANT),
        cost_estimate=cost(10_000_000_000, 36_000_000),
        name="build_send",
    )(info, own, sib)


def append(tail, given, take):
    def kern(take_ref, tail_ref, given_ref, out_ref, buf, sem):
        for m in range(TAIL):

            @pl.when(m < take_ref[0])
            def _():
                src = given_ref.at[:, pl.ds(m * TM, TM), :]
                dst = out_ref.at[:, pl.ds((TAIL - 1 - m) * TM, TM), :]
                cp = pltpu.make_async_copy(src, buf, sem)
                cp.start()
                cp.wait()
                cp = pltpu.make_async_copy(buf, dst, sem)
                cp.start()
                cp.wait()

    return pl.pallas_call(
        kern,
        in_specs=[SM, ANY, ANY],
        out_specs=ANY,
        out_shape=jax.ShapeDtypeStruct((2, TAIL * TM, D), BF),
        scratch_shapes=[pltpu.VMEM((2, TM, D), BF), pltpu.SemaphoreType.DMA],
        input_output_aliases={1: 0},
        compiler_params=pltpu.CompilerParams(vmem_limit_bytes=GRANT),
        cost_estimate=cost(1_000_000_000, 4_000_000),
        name="append",
    )(take, tail, given)


def gelu_and_slope(u):
    u2 = u * u
    t = jnp.tanh(u * (C1 + (C1 * C3) * u2))
    half = 0.5 + 0.5 * t
    act = u * half
    slope = half + (0.5 * u) * (1.0 - t * t) * (C1 + (3 * C1 * C3) * u2)
    return act, slope


def pick(e, lo, hi, fn):
    if hi - lo == 1:
        fn(lo)
        return
    mid = (lo + hi) // 2

    @pl.when(e < mid * 32)
    def _():
        pick(e, lo, mid, fn)

    @pl.when(e >= mid * 32)
    def _():
        pick(e, mid, hi, fn)


def issue_group(tab_ref, g, slot, src, xb, db, sem):
    for s in range(G):
        e = tab_ref[g * G + s]
        r = pl.multiple_of(lax.rem(e, 32) * TM, TM)

        def fetch(k):
            rows = pl.ds(s * TM, TM)
            pltpu.make_async_copy(src[k].at[0, pl.ds(r, TM), :], xb.at[slot, rows, :], sem.at[slot, 0]).start()
            pltpu.make_async_copy(src[k].at[1, pl.ds(r, TM), :], db.at[slot, rows, :], sem.at[slot, 1]).start()

        pick(e, 0, len(src), fetch)


def wait_group(slot, xb, db, sem):
    pltpu.make_async_copy(xb.at[slot], xb.at[slot], sem.at[slot, 0]).wait()
    pltpu.make_async_copy(db.at[slot], db.at[slot], sem.at[slot, 1]).wait()


def add_group(x, dy, wu, wd, gd, gu):
    u = lax.dot_general(wu[...], x, (((0,), (1,)), ((), ())), preferred_element_type=F32).astype(BF).astype(F32)
    da = lax.dot_general(wd[...], dy, (((1,), (1,)), ((), ())), preferred_element_type=F32)
    act, slope = gelu_and_slope(u)
    dh = (da * slope).astype(BF)
    gd[...] += jnp.dot(act.astype(BF), dy, preferred_element_type=F32)
    gu[...] += jnp.dot(dh, x, preferred_element_type=F32)


def weight_copies(c, lo, at, w, wub, wdb, sem):
    w_up, sib, fx, fd, w_down, wd_oth = w
    y, f = at
    xi, core = f // 2, f % 2
    cps = []
    c0, co = c * HB, (c - lo) * HB
    if not isinstance(c, int):
        c0, co = pl.multiple_of(c0, HB), pl.multiple_of(co, HB)
    for a in range(2):
        xa = xi if a == 0 else 1 - xi
        col = pl.multiple_of(((2 * xa + core) * 2 + y) * HALF + c0, HB)
        parts = [w_up.at[:, pl.ds(col, HB)], sib.at[a, :, pl.ds(c0, HB)]]
        parts += [ref.at[a, :, pl.ds(co, HB)] for ref in (fx, fd)]
        for k, part in enumerate(parts):
            rows = pl.ds(pl.multiple_of((f ^ k) * 512, 512), 512)
            cps.append(pltpu.make_async_copy(part, wub.at[rows, pl.ds(a * HB, HB)], sem.at[k, a]))
    own = pl.ds(pl.multiple_of(y * HALF + c0, HB), HB)
    cps.append(pltpu.make_async_copy(w_down.at[own, :], wdb.at[pl.ds(0, HB), :], sem.at[4, 0]))
    cps.append(pltpu.make_async_copy(wd_oth.at[pl.ds(co, HB), :], wdb.at[pl.ds(HB, HB), :], sem.at[4, 1]))
    return cps


def gather_scratch(n_acc):
    return [
        pltpu.VMEM((2, M, D), BF),
        pltpu.VMEM((2, M, D), BF),
        pltpu.VMEM((n_acc, D, FB), BF),
        pltpu.VMEM((n_acc, FB, D), BF),
        pltpu.VMEM((n_acc, FB, D), F32),
        pltpu.VMEM((n_acc, FB, D), F32),
        pltpu.SemaphoreType.DMA((2, 2)),
        pltpu.SemaphoreType.DMA((n_acc, 5, 2)),
    ]


def early_grads(tab, info, srcs, wsets, lo_chunk, n_new, prior=(), deps=()):
    ns, nw, npr = len(srcs), len(wsets), len(prior)
    sizes = [p[0].shape[0] for p in prior]
    n_chunks = n_new + sum(sizes)

    def kern(tab_ref, info_ref, *refs):
        src, refs = refs[:ns], refs[ns:]
        wrefs, refs = [refs[6 * k : 6 * k + 6] for k in range(nw)], refs[6 * nw :]
        pri, refs = refs[: 2 * npr], refs[2 * npr + len(deps) :]
        out_d, out_u, xb, db, wub, wdb, gd, gu, sem, wsem, asem = refs
        hi, at = info_ref[1], (info_ref[2], info_ref[3])

        def lo(q):
            return jnp.where(q < n_new, 0, info_ref[0])

        def weights(q, slot, act):
            c = jnp.where(q < n_new, lo_chunk + q, q - n_new) if npr else lo_chunk + q

            def act_all(k):
                for cp in weight_copies(c, wsets[k][0], at, wrefs[k], wub.at[slot], wdb.at[slot], wsem.at[slot]):
                    act(cp)

            if nw == 1:
                act_all(0)
                return
            for k in range(nw):
                first, count, _ = wsets[k]

                @pl.when(jnp.logical_and(c >= first, c < first + count))
                def _():
                    act_all(k)

        def start_copy(cp):
            cp.start()

        def wait_copy(cp):
            cp.wait()

        def results(q, slot):
            return (
                pltpu.make_async_copy(gd.at[slot], out_d.at[q], asem.at[slot, 0]),
                pltpu.make_async_copy(gu.at[slot], out_u.at[q], asem.at[slot, 1]),
            )

        issue_group(tab_ref, lo(0), 0, src, xb, db, sem)
        weights(0, 0, start_copy)

        def chunk(q, t):
            ws = lax.rem(q, 2)

            @pl.when(q + 1 < n_chunks)
            def _():
                weights(q + 1, 1 - ws, start_copy)

            @pl.when(q >= 2)
            def _():
                for cp in results(q - 2, ws):
                    cp.wait()

            @pl.when(q < n_new)
            def _():
                gd[ws] = jnp.zeros((FB, D), F32)
                gu[ws] = jnp.zeros((FB, D), F32)

            base = n_new
            for k in range(npr):
                first, base = base, base + sizes[k]

                @pl.when(jnp.logical_and(q >= first, q < base))
                def _():
                    cps = (
                        pltpu.make_async_copy(pri[2 * k].at[q - first], gd.at[ws], asem.at[ws, 0]),
                        pltpu.make_async_copy(pri[2 * k + 1].at[q - first], gu.at[ws], asem.at[ws, 1]),
                    )
                    for cp in cps:
                        cp.start()
                    for cp in cps:
                        cp.wait()

            weights(q, ws, wait_copy)

            def group(g, t):
                slot = lax.rem(t, 2)
                last = g + 1 == hi

                @pl.when(jnp.logical_or(jnp.logical_not(last), q + 1 < n_chunks))
                def _():
                    issue_group(tab_ref, jnp.where(last, lo(q + 1), g + 1), 1 - slot, src, xb, db, sem)

                wait_group(slot, xb, db, sem)
                add_group(xb[slot], db[slot], wub.at[ws], wdb.at[ws], gd.at[ws], gu.at[ws])
                return t + 1

            t = lax.fori_loop(lo(q), hi, group, t)
            for cp in results(q, ws):
                cp.start()
            return t

        lax.fori_loop(0, n_chunks, chunk, 0)
        for q in range(max(n_chunks - 2, 0), n_chunks):
            for cp in results(q, q % 2):
                cp.wait()

    flat = [a for _, _, w in wsets for a in w]
    pri = [a for p in prior for a in p]
    return pl.pallas_call(
        kern,
        in_specs=[SM, SM] + [ANY] * (ns + len(flat) + len(pri)) + [SM] * len(deps),
        out_specs=[ANY] * 2,
        out_shape=[jax.ShapeDtypeStruct((n_chunks, FB, D), F32)] * 2,
        scratch_shapes=gather_scratch(2) + [pltpu.SemaphoreType.DMA((2, 2))],
        compiler_params=pltpu.CompilerParams(vmem_limit_bytes=GRANT),
        cost_estimate=cost(8 * 5632 * D * FB * n_new, 60_000_000 * n_new),
    )(tab, info, *srcs, *flat, *pri, *deps)


def chunk_grads(j, tab, info, srcs, wset, prior, at, deps):
    ns = len(srcs)
    w_lo, _, w = wset

    def kern(tab_ref, info_ref, *refs):
        src, refs = refs[:ns], refs[ns:]
        wrefs, (pd, pu), refs = refs[:6], refs[6:8], refs[8 + len(deps) :]
        keep_d, send_d, keep_u, send_u, xb, db, wub, wdb, gd, gu, sem, wsem, osem = refs
        groups, y, f = info_ref[0], info_ref[1], info_ref[2]
        xi = f // 2
        wub, wdb, gd, gu = wub.at[0], wdb.at[0], gd.at[0], gu.at[0]

        @pl.when(groups > 0)
        def _():
            issue_group(tab_ref, 0, 0, src, xb, db, sem)

        cps = weight_copies(j, w_lo, (y, f), wrefs, wub, wdb, wsem.at[0])
        cps.append(pltpu.make_async_copy(pd.at[at], gd, osem.at[0]))
        cps.append(pltpu.make_async_copy(pu.at[at], gu, osem.at[1]))
        for cp in cps:
            cp.start()
        for cp in cps:
            cp.wait()

        def body(g, _):
            slot = lax.rem(g, 2)

            @pl.when(g + 1 < groups)
            def _():
                issue_group(tab_ref, g + 1, 1 - slot, src, xb, db, sem)

            wait_group(slot, xb, db, sem)
            add_group(xb[slot], db[slot], wub, wdb, gd, gu)
            return 0

        lax.fori_loop(0, groups, body, 0)
        kc = pl.multiple_of(xi * HALF, HALF)
        sc = pl.multiple_of((1 - xi) * HALF, HALF)
        ocp = [(gd.at[pl.ds(HB, HB), :], send_d), (gd.at[pl.ds(0, HB), :], keep_d)]
        for a in range(2):
            rows, cols = pl.ds(a * HB, HB), pl.ds(a * HALF, HALF)
            ocp.append((gu.at[rows, pl.ds(sc, HALF)], send_u.at[:, cols]))
            ocp.append((gu.at[rows, pl.ds(kc, HALF)], keep_u.at[:, cols]))
        ocp = [pltpu.make_async_copy(a, b, osem.at[i]) for i, (a, b) in enumerate(ocp)]
        for cp in ocp:
            cp.start()
        for cp in ocp:
            cp.wait()

    return pl.pallas_call(
        kern,
        in_specs=[SM, SM] + [ANY] * (ns + 8 + len(deps)),
        out_specs=[ANY] * 4,
        out_shape=[jax.ShapeDtypeStruct((HB, D), F32)] * 4,
        scratch_shapes=gather_scratch(1) + [pltpu.SemaphoreType.DMA((6,))],
        compiler_params=pltpu.CompilerParams(vmem_limit_bytes=GRANT),
        cost_estimate=cost(8 * 3072 * D * FB, 40_000_000),
    )(tab, info, *srcs, *w, *prior, *deps)


def finish_down(j, pos, keep, recv, out):
    first = out is None

    def kern(pos_ref, kd, rc, *refs):
        out_d, fd, vd, sem = refs if first else refs[1:]
        y = pos_ref[0]
        vd[...] = kd[...] + rc[...]
        row = pl.multiple_of(y * HALF + j * HB, HB)
        cps = [
            pltpu.make_async_copy(vd, fd, sem.at[0]),
            pltpu.make_async_copy(vd, out_d.at[pl.ds(row, HB), :], sem.at[1]),
        ]
        for cp in cps:
            cp.start()
        for cp in cps:
            cp.wait()

    extra = [] if first else [out]
    return pl.pallas_call(
        kern,
        in_specs=[SM, VM, VM] + [ANY] * len(extra),
        out_specs=[ANY] * 2,
        out_shape=[jax.ShapeDtypeStruct((D, D), F32), jax.ShapeDtypeStruct((HB, D), F32)],
        scratch_shapes=[pltpu.VMEM((HB, D), F32), pltpu.SemaphoreType.DMA((2,))],
        input_output_aliases={} if first else {3: 0},
        compiler_params=pltpu.CompilerParams(vmem_limit_bytes=GRANT),
        cost_estimate=cost(2_000_000_000, 4_000_000),
    )(pos, keep, recv, *extra)


def finish_up(j, pos, keep, recv, out):
    first = out is None

    def kern(pos_ref, ku, rc, *refs):
        out_u, fuc, fus, vu, sem = refs if first else refs[1:]
        y, xi, c = pos_ref[0], pos_ref[1], pos_ref[2]
        mine = pl.ds(pl.multiple_of(c * 512, 512), 512)
        other = pl.ds(pl.multiple_of((1 - c) * 512, 512), 512)
        vu[0] = (ku[:, 0:HALF] + rc[:, HALF:D]).T
        vu[1] = (ku[:, HALF:D] + rc[:, 0:HALF]).T
        cps = [
            pltpu.make_async_copy(vu.at[:, other, :], fus, sem.at[0]),
            pltpu.make_async_copy(vu.at[:, mine, :], fuc, sem.at[1]),
        ]
        for a in range(2):
            xa = xi if a == 0 else 1 - xi
            col = pl.multiple_of(((2 * xa + c) * 2 + y) * HALF + j * HB, HB)
            cps.append(pltpu.make_async_copy(vu.at[a, mine, :], out_u.at[:, pl.ds(col, HB)], sem.at[2 + a]))
        for cp in cps:
            cp.start()
        for cp in cps:
            cp.wait()

    extra = [] if first else [out]
    return pl.pallas_call(
        kern,
        in_specs=[SM, VM, VM] + [ANY] * len(extra),
        out_specs=[ANY] * 3,
        out_shape=[
            jax.ShapeDtypeStruct((512, 4 * D), F32),
            jax.ShapeDtypeStruct((2, 512, HB), F32),
            jax.ShapeDtypeStruct((2, 512, HB), F32),
        ],
        scratch_shapes=[pltpu.VMEM((2, HALF, HB), F32), pltpu.SemaphoreType.DMA((4,))],
        input_output_aliases={} if first else {3: 0},
        compiler_params=pltpu.CompilerParams(vmem_limit_bytes=GRANT),
        cost_estimate=cost(2_000_000_000, 4_000_000),
    )(pos, keep, recv, *extra)


def store(j, pos, rd, ruc, ruy, rus, outs):
    def kern(pos_ref, d_ref, uc_ref, uy_ref, us_ref, _d, _u, out_d, out_u, vd, vu, isem, osem):
        y, xi, c = pos_ref[0], pos_ref[1], pos_ref[2]
        row = pl.multiple_of((1 - y) * HALF + j * HB, HB)
        work = [(d_ref, vd, [(vd, out_d.at[pl.ds(row, HB), :])])]
        for k, (ref, cc, yy) in enumerate(((uc_ref, c, 1 - y), (uy_ref, 1 - c, 1 - y), (us_ref, 1 - c, y))):
            puts = []
            for a in range(2):
                xa = xi if a == 0 else 1 - xi
                col = pl.multiple_of(((2 * xa + cc) * 2 + yy) * HALF + j * HB, HB)
                puts.append((vu.at[k, a], out_u.at[:, pl.ds(col, HB)]))
            work.append((ref, vu.at[k], puts))
        loads = [pltpu.make_async_copy(src, mid, isem.at[n]) for n, (src, mid, _) in enumerate(work)]
        for cp in loads:
            cp.start()
        done = []
        for cp, (_, _, puts) in zip(loads, work):
            cp.wait()
            for src, dst in puts:
                put = pltpu.make_async_copy(src, dst, osem.at[len(done)])
                put.start()
                done.append(put)
        for put in done:
            put.wait()

    return pl.pallas_call(
        kern,
        in_specs=[SM] + [ANY] * 6,
        out_specs=[ANY] * 2,
        out_shape=[jax.ShapeDtypeStruct((D, D), F32), jax.ShapeDtypeStruct((512, 4 * D), F32)],
        scratch_shapes=[
            pltpu.VMEM((HB, D), F32),
            pltpu.VMEM((3, 2, 512, HB), F32),
            pltpu.SemaphoreType.DMA((4,)),
            pltpu.SemaphoreType.DMA((7,)),
        ],
        input_output_aliases={5: 0, 6: 1},
        compiler_params=pltpu.CompilerParams(vmem_limit_bytes=16 * MIB),
        cost_estimate=cost(3_000_000_000, 5_000_000),
    )(pos, rd, ruc, ruy, rus, *outs)


def nothing(k):
    return pl.pallas_call(lambda o: None, out_specs=ANY, out_shape=jax.ShapeDtypeStruct((2, k * TM, D), BF))()


def exchange_branch(parts, early):
    here = [k in parts for k in range(len(MAIN))]

    def run(pieces, tail, give, take, *rest):
        got = []
        for k in range(len(MAIN)):
            got.append(y_swap(pieces[k]) if here[k] else nothing(MAIN[k]))
        given = x_swap(give)
        acc = early(0, *rest)
        given_s = core_swap(given)
        tail = append(tail, given, take)
        last = y_swap(tail)
        acc = (*acc, *early(1, *rest))
        sib = []
        for k in range(len(MAIN)):
            sib.append(core_swap(got[k]) if here[k] else nothing(MAIN[k]))
        last_s = core_swap(last)
        return (*got, last, *sib, last_s, given, given_s, *acc)

    return run


def piece_starts():
    table = []
    for size, parts in zip(SIZES, PARTS):
        at, row = FIRST, []
        for k in range(len(MAIN)):
            row.append(at)
            at += MAIN[k] if k in parts else 0
        assert at + TAIL == FIRST + size
        table.append([*row, at])
    return table


def solution(mesh):
    tok_spec = P(None, ("model", "replica", "fsdp"), None)
    len_spec = P(None, ("model", "replica", "fsdp"))
    w_spec = P(None, ("model", "fsdp"), None)

    def group_grads(x_in, dy, lengths, w_up, w_down):
        y, f = lax.axis_index("replica"), lax.axis_index("fsdp")
        xi, c = f // 2, f % 2
        w_up, w_down = w_up[0], w_down[0]

        row = jnp.zeros((8, 128), jnp.int32).at[0, :MICRO].set(lengths[:, 0].astype(jnp.int32))
        around, s1 = start(row, x_in, dy)
        s1 = s1.reshape(2, MICRO * BASE, D)
        s1_y = y_swap(s1)

        def cols(xd, cd, lo=0, n=HALF):
            own = lax.dynamic_slice(w_up, (0, ((2 * xd + cd) * 2 + y) * HALF + lo), (512, n))
            oth = lax.dynamic_slice(w_up, (0, ((2 * (1 - xd) + cd) * 2 + y) * HALF + lo), (512, n))
            return jnp.stack([own, oth])

        from_s = core_swap(cols(xi, 1 - c))
        wsets = []
        for lo, n in WSETS:
            a = x_swap(cols(1 - xi, c, lo * HB, n * HB))
            b = x_diag(cols(1 - xi, 1 - c, lo * HB, n * HB))
            d = x_swap(lax.dynamic_slice(w_down, (y * HALF + lo * HB, 0), (n * HB, D)))
            wsets.append((lo, n, [w_up, from_s, a, b, w_down, d]))

        todo = plan(around)
        packed = pack_rest(x_in, dy, todo["rest"], todo["offs"])
        packed_s = core_swap(packed)
        s1_s = core_swap(s1)
        pa, *pieces, tail, give = build_send(packed, packed_s, todo["send"])
        qa = y_swap(pa)

        own_srcs = (s1, s1_s, packed, packed_s)
        tab, late, info_late, pos = (todo[k] for k in ("tab", "late", "info", "pos"))
        acc0 = early_grads(tab, todo["own"], own_srcs, wsets[:1], 0, 2)
        acc1 = early_grads(tab, todo["own"], own_srcs, wsets[1:2], 2, 1)
        s1_ys = core_swap(s1_y)
        srcs = (*own_srcs, s1_y, s1_ys)
        acc2 = early_grads(tab, todo["every"], srcs, wsets[1:2], 3, 1)

        def early(step, tab, info, srcs, w, prior):
            sets = [(lo, n, v) for (lo, n), v in zip(WSETS, w)]
            if step == 0:
                return early_grads(tab, info, srcs, sets[2:], 4, 2)
            return early_grads(tab, info, srcs, sets, 6, 2, prior)

        got = lax.switch(
            todo["which"][0],
            [exchange_branch(parts, early) for parts in PARTS],
            pieces, tail, give, todo["take"],
            tab, todo["every"], srcs, [w for _, _, w in wsets], [list(acc0), list(acc1)],
        )
        k = len(MAIN) + 1
        pieces, sib_pieces, given, acc3, acc4 = got[:k], got[k : 2 * k], got[2 * k : 2 * k + 2], got[-4:-2], got[-2:]
        qas = core_swap(qa)
        srcs = (qa, *pieces, qas, *sib_pieces, *given, packed)
        prior = [(acc4, 2), (acc4, 3), (acc4, 4), (acc2, 0), (acc3, 0), (acc3, 1), (acc4, 0), (acc4, 1)]

        out_d = out_u = None
        fin = []
        for p, j in enumerate(ORDER):
            deps = (fin[p - 2][0],) if p >= 2 else ()
            w_at = next(h for h, (lo, n) in enumerate(WSETS) if lo <= j < lo + n)
            keep_d, send_d, keep_u, send_u = chunk_grads(
                j, late, info_late, srcs, wsets[w_at], *prior[j], deps
            )
            recv_d = x_swap(send_d)
            recv_u = x_swap(send_u)
            out_d, fd = finish_down(j, pos, keep_d, recv_d, out_d)
            rd = y_swap(fd)
            if p >= LAG:
                out_d, out_u = store(ORDER[p - LAG], pos, *fin[p - LAG][1], (out_d, out_u))
            out_u, fuc, fus = finish_up(j, pos, keep_u, recv_u, out_u)
            ruc = y_swap(fuc)
            ruy = y_diag(fus)
            rus = core_swap(fus)
            fin.append((fuc, (rd, ruc, ruy, rus)))
        for p in range(NCH - LAG, NCH):
            out_d, out_u = store(ORDER[p], pos, *fin[p][1], (out_d, out_u))
        return out_u[None], out_d[None]


    return jax.shard_map(
        group_grads,
        mesh=mesh,
        in_specs=(tok_spec, tok_spec, len_spec, w_spec, w_spec),
        out_specs=(w_spec, w_spec),
        check_vma=False,
    )
```
